512 devices in a mesh: gx: 64 (over x, z, y_hi), gy: 8 (over y_lo, core).
Axes of the slice: x: 4, y: 8 (y_hi: 2, y_lo: 4; y = y_hi * 4 + y_lo), z: 8, core: 2. Of those that a mesh axis runs over, the one named last changes fastest.
Arguments:
- moisture_ratio: float32 [2, 512, 1024], P(None, 'gx', 'gy'), may hold values from 11 to 14
- kelvin_warmth: float32 [2, 512, 1024], P(None, 'gx', 'gy'), may hold values from 286 to 292
- droplet_size_micron: float32 [8, 2, 512, 1024], P(None, None, 'gx', 'gy'), may hold values from 0.5 to 25
- weighting_factor: float32 [8, 2, 512, 1024], P(None, None, 'gx', 'gy'), may hold values from 0.1 to 2
- dry_nucleus_size: float32 [8, 2, 512, 1024], P(None, None, 'gx', 'gy'), may hold values from 0.02 to 0.3
- fractional_offset_east: float32 [8, 2, 512, 1024], P(None, None, 'gx', 'gy'), may hold values from 0 to 1
- fractional_offset_north: float32 [8, 2, 512, 1024], P(None, None, 'gx', 'gy'), may hold values from 0 to 1
- encounter_permutation: int32 [8, 2, 512, 1024], P(None, None, 'gx', 'gy'), may hold values from 0 to 7, as said below
- departing_eastwest_lists: int32 [64, 2, 8192], P('gx', None, 'gy'), may hold values from -1 to 16383, as said below
- departing_northsouth_lists: int32 [64, 2, 384], P('gx', None, 'gy'), may hold values from -1 to 16383, as said below
- departing_diagonal_lists: int32 [64, 4, 64], P('gx', None, 'gy'), may hold values from -1 to 16383, as said below
Outputs:
- resulting_moisture_ratio: float32 [2, 512, 1024], P(None, 'gx', 'gy')
- resulting_kelvin_value: float32 [2, 512, 1024], P(None, 'gx', 'gy')
- resulting_droplet_size: float32 [8, 2, 512, 1024], P(None, None, 'gx', 'gy')
- resulting_weighting_factor: float32 [8, 2, 512, 1024], P(None, None, 'gx', 'gy')
- arrival_particle_records: float32 [5, 64, 17408], P(None, 'gx', 'gy')
- arrival_box_index: int32 [64, 17408], P('gx', 'gy')
The draws below stay inside these ranges and needn't reach their ends.
Inputs may be any that keep to these rules, and one draw needn't show every extreme that they name: `encounter_permutation`: along the first dimension, the 8 entries of each cell are a permutation of 0 to 7. `departing_eastwest_lists`: each list holds live slot numbers of its own device first and -1 after them, at most 1024 live, and some list of some device is full. Row 0 names only droplets of cells with i = 7, row 1 only i = 0, both only 0 < j < 127. No slot is named twice among all lists of a device. `departing_northsouth_lists`: each list holds live slot numbers of its own device first and -1 after them, at most 48 live, and some list of some device is full. Row 0 names only droplets of cells with j = 127, row 1 only j = 0, both only 0 < i < 7. `departing_diagonal_lists`: each list holds live slot numbers of its own device first and -1 after them, at most 8 live, and some list of some device is full. Row r names only droplets of the corner cell that its move points to: i = 7 for rows 0 and 1, i = 0 for rows 2 and 3, j = 127 for rows 0 and 2, j = 0 for rows 1 and 3.
All inputs are finite; a program needn't handle non-finite values.
Results may differ from the reference program's by a relative error of at most 0.0003.
Values sent between devices are 32-bit elements; how exact they have to be, the bound alone decides.
No kernel may reach another device: no remote copies, remote signals or barrier semaphores. Data moves between devices by JAX's collectives and lax.ppermute only.
A program may use at most 64 MiB of HBM per device.

```python
import math
import jax
import jax.numpy as jnp
from jax import lax

NUMBER_OF_TIERS = 2
SD = 8
NEWTON = 4
CX = 8
CY = 128
GRID_WIDTH_EAST = 512
GRID_WIDTH_NORTH = 1024
DROPS = 16384
KX = 1024
KY = 48
KC = 8
NARR = 2176
N_GX = 64
N_GY = 8


def draw_lists(key, list_rows, list_length, eligible, slot_of):
    grid_x = GRID_WIDTH_EAST // CX
    grid_y = GRID_WIDTH_NORTH // CY
    total_lists = grid_x * list_rows * grid_y
    keys = jax.random.split(key, total_lists)
    chosen = jax.vmap(lambda single: jax.random.permutation(single, eligible)[:list_length])(keys)
    chosen = chosen.reshape(grid_x, list_rows, grid_y, list_length).astype(jnp.int32)
    direction = lax.broadcasted_iota(jnp.int32, chosen.shape, 1)
    slots = slot_of(chosen, direction).astype(jnp.int32)
    live_count = jax.random.randint(jax.random.fold_in(key, 1), (grid_x, list_rows, grid_y, 1), list_length // 4, list_length + 1)
    fullest = jax.random.randint(jax.random.fold_in(key, 2), (), 0, total_lists)
    list_id = (lax.broadcasted_iota(jnp.int32, live_count.shape, 0) * list_rows + lax.broadcasted_iota(jnp.int32, live_count.shape, 1)) * grid_y + lax.broadcasted_iota(jnp.int32, live_count.shape, 2)
    live_count = jnp.where(list_id == fullest, list_length, live_count)
    position = lax.broadcasted_iota(jnp.int32, chosen.shape, 3)
    result = jnp.where(position < live_count, slots, -1)
    return result.reshape(grid_x, list_rows, grid_y * list_length).astype(jnp.int32)


def draw_departing_eastwest_lists(key, part):
    inner_width = CY - 2

    def slot_of(chosen, direction):
        stack_level = chosen // inner_width
        index_y = chosen % inner_width + 1
        index_x = jnp.where(direction == 0, CX - 1, 0)
        return (stack_level * CX + index_x) * CY + index_y
    return draw_lists(jax.random.fold_in(key, 11), 2, KX, SD * NUMBER_OF_TIERS * inner_width, slot_of)


def draw_departing_northsouth_lists(key, part):
    inner_width = CX - 2

    def slot_of(chosen, direction):
        stack_level = chosen // inner_width
        index_x = chosen % inner_width + 1
        index_y = jnp.where(direction == 0, CY - 1, 0)
        return (stack_level * CX + index_x) * CY + index_y
    return draw_lists(jax.random.fold_in(key, 12), 2, KY, SD * NUMBER_OF_TIERS * inner_width, slot_of)


def draw_departing_diagonal_lists(key, part):

    def slot_of(chosen, direction):
        index_x = jnp.where(direction < 2, CX - 1, 0)
        index_y = jnp.where(direction % 2 == 0, CY - 1, 0)
        return (chosen * CX + index_x) * CY + index_y
    return draw_lists(jax.random.fold_in(key, 13), 4, KC, SD * NUMBER_OF_TIERS, slot_of)


def draw_encounter_permutation(key, part):
    shape_all = (SD, NUMBER_OF_TIERS, GRID_WIDTH_EAST, GRID_WIDTH_NORTH)
    scores = jax.random.randint(jax.random.fold_in(key, 14), shape_all, 0, 1 << 20) * SD + lax.broadcasted_iota(jnp.int32, shape_all, 0)
    return jnp.argsort(scores, axis=0).astype(jnp.int32)


def block_scale(own_key, extent, cuts, smallest, largest):
    level = 1.0
    for axis_at, blocks in cuts:
        steps = jax.random.uniform(jax.random.fold_in(jax.random.fold_in(own_key, 6), axis_at), (blocks,), jnp.float32, smallest / len(cuts), largest / len(cuts))
        level = level * jnp.repeat(jnp.exp(steps), extent[axis_at] // blocks).reshape((-1,) + (1,) * (len(extent) - 1 - axis_at))
    return level


def setup_inputs(seed: int = 0) -> dict:
    seeds = jax.random.split(jax.random.key(seed), 12)
    return {
        "moisture_ratio": jnp.clip(11.0 + 3.0 * jax.random.uniform(seeds[0], (NUMBER_OF_TIERS, GRID_WIDTH_EAST, GRID_WIDTH_NORTH), jnp.float32) ** block_scale(seeds[0], (NUMBER_OF_TIERS, GRID_WIDTH_EAST, GRID_WIDTH_NORTH), ((1, 64), (2, 8)), -0.2, 0.2), 11.0, 14.0),
        "kelvin_warmth": jnp.clip(286.0 + 6.0 * jax.random.uniform(seeds[1], (NUMBER_OF_TIERS, GRID_WIDTH_EAST, GRID_WIDTH_NORTH), jnp.float32) ** block_scale(seeds[1], (NUMBER_OF_TIERS, GRID_WIDTH_EAST, GRID_WIDTH_NORTH), ((1, 64), (2, 8)), -0.2, 0.2), 286.0, 292.0),
        "droplet_size_micron": jnp.clip(jnp.exp(math.log(25.0) - 3.912023 * jax.random.uniform(seeds[2], (SD, NUMBER_OF_TIERS, GRID_WIDTH_EAST, GRID_WIDTH_NORTH), jnp.float32) ** block_scale(seeds[2], (SD, NUMBER_OF_TIERS, GRID_WIDTH_EAST, GRID_WIDTH_NORTH), ((2, 64), (3, 8)), -0.2, 0.2)), 0.5, 25.0),
        "weighting_factor": jnp.clip(jnp.exp(math.log(2.0) - 2.9957323 * jax.random.uniform(seeds[3], (SD, NUMBER_OF_TIERS, GRID_WIDTH_EAST, GRID_WIDTH_NORTH), jnp.float32) ** block_scale(seeds[3], (SD, NUMBER_OF_TIERS, GRID_WIDTH_EAST, GRID_WIDTH_NORTH), ((2, 64), (3, 8)), -0.2, 0.2)), 0.1, 2.0),
        "dry_nucleus_size": jnp.clip(jnp.exp(math.log(0.3) - 2.7080503 * jax.random.uniform(seeds[4], (SD, NUMBER_OF_TIERS, GRID_WIDTH_EAST, GRID_WIDTH_NORTH), jnp.float32) ** block_scale(seeds[4], (SD, NUMBER_OF_TIERS, GRID_WIDTH_EAST, GRID_WIDTH_NORTH), ((2, 64), (3, 8)), -0.2, 0.2)), 0.02, 0.3),
        "fractional_offset_east": jnp.clip(1.0 * jax.random.uniform(seeds[5], (SD, NUMBER_OF_TIERS, GRID_WIDTH_EAST, GRID_WIDTH_NORTH), jnp.float32) ** block_scale(seeds[5], (SD, NUMBER_OF_TIERS, GRID_WIDTH_EAST, GRID_WIDTH_NORTH), ((2, 64), (3, 8)), -0.2, 0.2), 0.0, 1.0),
        "fractional_offset_north": jnp.clip(1.0 * jax.random.uniform(seeds[6], (SD, NUMBER_OF_TIERS, GRID_WIDTH_EAST, GRID_WIDTH_NORTH), jnp.float32) ** block_scale(seeds[6], (SD, NUMBER_OF_TIERS, GRID_WIDTH_EAST, GRID_WIDTH_NORTH), ((2, 64), (3, 8)), -0.2, 0.2), 0.0, 1.0),
        "encounter_permutation": draw_encounter_permutation(jax.random.fold_in(seeds[11], 71), 0),
        "departing_eastwest_lists": draw_departing_eastwest_lists(jax.random.fold_in(seeds[11], 71), 0),
        "departing_northsouth_lists": draw_departing_northsouth_lists(jax.random.fold_in(seeds[11], 71), 0),
        "departing_diagonal_lists": draw_departing_diagonal_lists(jax.random.fold_in(seeds[11], 71), 0),
    }


MIX_HORIZONTAL = 0.2
MIX_VERTICAL = 0.05
EXCESS_FACTOR = 4.2222
CURVATURE = 0.0012
KAPPA_SOLUTE = 0.6
GROWTH_STEP = 200.0
COLLIDE_RATE = 4e-07
VAPOUR_PER_SOURCE = 0.001
WARMING_FACTOR = 0.00249

def moisture_excess(moisture_ratio, kelvin_warmth):
    maximum_list_length = EXCESS_FACTOR * jnp.exp(17.27 * (kelvin_warmth - 273.15) / (kelvin_warmth - 35.86))
    return moisture_ratio / maximum_list_length - 1.0

def kernel_weights(offset):
    return (jnp.maximum(0.5 - offset, 0.0), 1.0 - jnp.abs(offset - 0.5), jnp.maximum(offset - 0.5, 0.0))

def vertical_mix(centre, level_axis):
    levels = centre.shape[level_axis]
    above = jnp.concatenate([lax.slice_in_dim(centre, 1, levels, axis=level_axis), lax.slice_in_dim(centre, levels - 1, levels, axis=level_axis)], level_axis)
    below = jnp.concatenate([lax.slice_in_dim(centre, 0, 1, axis=level_axis), lax.slice_in_dim(centre, 0, levels - 1, axis=level_axis)], level_axis)
    return above + below - 2.0 * centre

def domain_wide_stirring(field):
    horizontal = jnp.roll(field, 1, 1) + jnp.roll(field, -1, 1) + jnp.roll(field, 1, 2) + jnp.roll(field, -1, 2) - 4.0 * field
    return field + MIX_HORIZONTAL * horizontal + MIX_VERTICAL * vertical_mix(field, 0)

def grow_droplets(droplet_size_micron, dry_nucleus_size, forcing):
    initial = droplet_size_micron * droplet_size_micron
    solute = KAPPA_SOLUTE * dry_nucleus_size * dry_nucleus_size * dry_nucleus_size
    lowest = dry_nucleus_size * dry_nucleus_size
    wetted = initial
    for sweep in range(NEWTON):
        root_wet = jnp.sqrt(wetted)
        inverse = 1.0 / (wetted * root_wet)
        residue = wetted - initial - GROWTH_STEP * (forcing + solute * inverse)
        slope_value = 1.0 + 1.5 * GROWTH_STEP * solute * inverse / wetted
        wetted = jnp.maximum(wetted - residue / slope_value, lowest)
    return wetted

def coalesce(grown_radius, weighting_factor, encounter_permutation):
    ordered_radius = jnp.take_along_axis(grown_radius, encounter_permutation, axis=0)
    ordered_mult = jnp.take_along_axis(weighting_factor, encounter_permutation, axis=0)
    first_radius = ordered_radius[0::2]
    second_radius = ordered_radius[1::2]
    first_mult = ordered_mult[0::2]
    second_mult = ordered_mult[1::2]
    first_big = first_mult >= second_mult
    high_radius = jnp.where(first_big, first_radius, second_radius)
    low_radius = jnp.where(first_big, second_radius, first_radius)
    high_mult = jnp.where(first_big, first_mult, second_mult)
    low_mult = jnp.where(first_big, second_mult, first_mult)
    radius_sum = first_radius + second_radius
    kernel = COLLIDE_RATE * high_mult * radius_sum * radius_sum * jnp.abs(first_radius * first_radius - second_radius * second_radius)
    chance = 1.0 - jnp.exp(-kernel)
    merged_radius = jnp.cbrt(low_radius * low_radius * low_radius + chance * high_radius * high_radius * high_radius)
    reduced_mult = high_mult - chance * low_mult
    new_first_radius = jnp.where(first_big, high_radius, merged_radius)
    new_second_radius = jnp.where(first_big, merged_radius, high_radius)
    new_first_mult = jnp.where(first_big, reduced_mult, low_mult)
    new_second_mult = jnp.where(first_big, low_mult, reduced_mult)
    paired_radius = jnp.stack([new_first_radius, new_second_radius], 1).reshape(grown_radius.shape)
    paired_mult = jnp.stack([new_first_mult, new_second_mult], 1).reshape(grown_radius.shape)
    positions = lax.broadcasted_iota(jnp.int32, encounter_permutation.shape, 0)
    ranks = []
    for target in range(encounter_permutation.shape[0]):
        ranks.append(lax.optimization_barrier(jnp.sum(jnp.where(encounter_permutation == target, positions, 0), axis=0)))
    slot_rank = jnp.stack(ranks, 0).astype(jnp.int32)
    return (jnp.take_along_axis(paired_radius, slot_rank, axis=0), jnp.take_along_axis(paired_mult, slot_rank, axis=0))

def to_blocks(values):
    return values.reshape(SD, NUMBER_OF_TIERS, N_GX, CX, N_GY, CY).transpose(2, 4, 0, 1, 3, 5).reshape(N_GX, N_GY, DROPS)

def from_blocks(values):
    return values.reshape(N_GX, N_GY, SD, NUMBER_OF_TIERS, CX, CY).transpose(2, 3, 0, 4, 1, 5).reshape(SD, NUMBER_OF_TIERS, N_GX * CX, N_GY * CY)

def list_blocks(lists, list_rows, list_length):
    return lists.reshape(N_GX, list_rows, N_GY, list_length).transpose(0, 2, 1, 3)

def make_records(attr_table, lists, directions):
    list_rows = lists.shape[2]
    list_length = lists.shape[3]
    is_live = lists >= 0
    safe_slot = jnp.where(is_live, lists, 0).astype(jnp.int32)
    take_index = jnp.broadcast_to(safe_slot.reshape(N_GX, N_GY, 1, list_rows * list_length), (N_GX, N_GY, 5, list_rows * list_length))
    picked = jnp.take_along_axis(attr_table, take_index, axis=3)
    picked = picked.reshape(N_GX, N_GY, 5, list_rows, list_length).transpose(0, 1, 3, 2, 4)
    picked = jnp.where(is_live[:, :, :, None, :], picked, 0.0)
    cell_index = safe_slot % (NUMBER_OF_TIERS * CX * CY)
    level_index = cell_index // (CX * CY)
    index_x = cell_index // CY % CX
    index_y = cell_index % CY
    move_x = jnp.array([entry[0] for entry in directions], jnp.int32).reshape(1, 1, list_rows, 1)
    move_y = jnp.array([entry[1] for entry in directions], jnp.int32).reshape(1, 1, list_rows, 1)
    target = (level_index * CX + (index_x + move_x) % CX) * CY + (index_y + move_y) % CY
    target = jnp.where(is_live, target, -1).astype(attr_table.dtype)
    return jnp.concatenate([picked, target[:, :, :, None, :]], 3)

def reference(moisture_ratio, kelvin_warmth, droplet_size_micron, weighting_factor, dry_nucleus_size, fractional_offset_east, fractional_offset_north, encounter_permutation, departing_eastwest_lists, departing_northsouth_lists, departing_diagonal_lists):
    averaged_moisture_ratio = domain_wide_stirring(moisture_ratio)
    averaged_warmth_kelvin = domain_wide_stirring(kelvin_warmth)
    moisture_fraction = moisture_excess(averaged_moisture_ratio, averaged_warmth_kelvin)
    weight_x = kernel_weights(fractional_offset_east)
    weight_y = kernel_weights(fractional_offset_north)
    forcing = jnp.zeros_like(droplet_size_micron)
    for shift_x in range(3):
        for shift_y in range(3):
            shifted = jnp.roll(moisture_fraction, (1 - shift_x, 1 - shift_y), (1, 2))
            forcing = forcing + weight_x[shift_x] * weight_y[shift_y] * shifted[None]
    forcing = forcing - CURVATURE / droplet_size_micron
    wetted = grow_droplets(droplet_size_micron, dry_nucleus_size, forcing)
    condensed = weighting_factor * (wetted * jnp.sqrt(wetted) - droplet_size_micron * droplet_size_micron * droplet_size_micron)
    deposition_rate_term = jnp.zeros_like(moisture_ratio)
    for shift_x in range(3):
        for shift_y in range(3):
            deposit = lax.optimization_barrier(jnp.sum(weight_x[shift_x] * weight_y[shift_y] * condensed, axis=0))
            deposition_rate_term = deposition_rate_term + jnp.roll(deposit, (shift_x - 1, shift_y - 1), (1, 2))
    resulting_moisture_ratio = averaged_moisture_ratio - VAPOUR_PER_SOURCE * deposition_rate_term
    resulting_kelvin_value = averaged_warmth_kelvin + WARMING_FACTOR * deposition_rate_term
    grown_radius = jnp.sqrt(wetted)
    resulting_droplet_size, coalesced = coalesce(grown_radius, weighting_factor, encounter_permutation)
    lists_x = list_blocks(departing_eastwest_lists, 2, KX)
    lists_y = list_blocks(departing_northsouth_lists, 2, KY)
    lists_corner = list_blocks(departing_diagonal_lists, 4, KC)
    all_lists = jnp.concatenate([lists_x.reshape(N_GX, N_GY, -1), lists_y.reshape(N_GX, N_GY, -1), lists_corner.reshape(N_GX, N_GY, -1)], 2)
    grid_first = lax.broadcasted_iota(jnp.int32, all_lists.shape, 0)
    grid_second = lax.broadcasted_iota(jnp.int32, all_lists.shape, 1)
    whole_count = N_GX * N_GY * DROPS
    flat_slot = jnp.where(all_lists >= 0, (grid_first * N_GY + grid_second) * DROPS + all_lists, whole_count)
    departed = jnp.zeros((whole_count,), droplet_size_micron.dtype).at[flat_slot.reshape(-1)].set(1.0, mode='drop')
    departed = from_blocks(departed.reshape(N_GX, N_GY, DROPS))
    resulting_weighting_factor = jnp.where(departed > 0.0, 0.0, coalesced)
    attr_table = jnp.stack([to_blocks(resulting_droplet_size), to_blocks(coalesced), to_blocks(dry_nucleus_size), to_blocks(fractional_offset_east), to_blocks(fractional_offset_north)], 2)
    records_x = make_records(attr_table, lists_x, ((1, 0), (-1, 0)))
    records_y = make_records(attr_table, lists_y, ((0, 1), (0, -1)))
    records_corner = make_records(attr_table, lists_corner, ((1, 1), (1, -1), (-1, 1), (-1, -1)))
    from_west = jnp.roll(records_x[:, :, 0], 1, 0)
    from_east = jnp.roll(records_x[:, :, 1], -1, 0)
    from_south = jnp.roll(records_y[:, :, 0], 1, 1)
    from_north = jnp.roll(records_y[:, :, 1], -1, 1)
    south_west = jnp.roll(records_corner[:, :, 0], (1, 1), (0, 1))
    south_east = jnp.roll(records_corner[:, :, 2], (-1, 1), (0, 1))
    north_west = jnp.roll(records_corner[:, :, 1], (1, -1), (0, 1))
    north_east = jnp.roll(records_corner[:, :, 3], (-1, -1), (0, 1))
    arrivals = jnp.concatenate([from_west, from_east, from_south, from_north, south_west, south_east, north_west, north_east], 3)
    arrival_particle_records = arrivals[:, :, :5].transpose(2, 0, 1, 3).reshape(5, N_GX, N_GY * NARR)
    arrival_box_index = arrivals[:, :, 5].astype(jnp.int32).reshape(N_GX, N_GY * NARR)
    return (resulting_moisture_ratio, resulting_kelvin_value, resulting_droplet_size, resulting_weighting_factor, arrival_particle_records, arrival_box_index)
```

```python
import jax
import jax.numpy as jnp
from jax import lax
from jax.experimental import pallas as pl
from jax.experimental.pallas import tpu as pltpu
from jax.sharding import PartitionSpec as P


NEWTON = 4
MIX_HORIZONTAL = 0.2
MIX_VERTICAL = 0.05
EXCESS_FACTOR = 4.2222
CURVATURE = 0.0012
KAPPA_SOLUTE = 0.6
GROWTH_STEP = 200.0
COLLIDE_RATE = 4e-07
VAPOUR_PER_SOURCE = 0.001
WARMING_FACTOR = 0.00249

F32 = jnp.float32
I32 = jnp.int32
SD = 8
FIELDS = 6

G_AIR = 0
G_DROP = 32
G_LIST = 80
G_ROWS = 88
X_DROP = 0
X_AIR = 96
X_EXT = 128
X_CORNER = 160
X_LIST = 208
X_SMALL = 216
X_ROWS = 224


def lanes_of(shape):
    return lax.broadcasted_iota(I32, shape, len(shape) - 1)


def rows_of(shape):
    return lax.broadcasted_iota(I32, shape, len(shape) - 2)


def pack_gy_kernel(q_ref, t_ref, sz_ref, wt_ref, dn_ref, ox_ref, oy_ref, pm_ref, small_ref, g_ref):
    g_ref[G_AIR : G_AIR + 16, :] = q_ref[...]
    g_ref[G_AIR + 16 : G_AIR + 32, :] = t_ref[...]
    lane = lanes_of((8, 128))
    first = lane < 32
    low_level = lane % 32 < 16
    for f, ref in enumerate((sz_ref, wt_ref, dn_ref, ox_ref, oy_ref, pm_ref)):
        parts = [ref[k * 16 : k * 16 + 16, :] for k in range(SD - 1, -1, -1)]
        block = jnp.concatenate(parts, 0)
        if f == 5:
            block = block.astype(F32)
        turned = jnp.transpose(block)
        sides = []
        for row in (127, 0):
            line = jnp.broadcast_to(turned[row : row + 1, :], (8, 128))
            sides.append(line)
        out = []
        for n, line in enumerate(sides):
            base = 32 * n
            line = pltpu.roll(line, 16, 1, stride=16, stride_axis=0)
            lev0 = pltpu.roll(line, base + 4, 1)
            lev1 = pltpu.roll(line, base + 12, 1)
            out.append(jnp.where(low_level, lev0, lev1))
        g_ref[G_DROP + f * 8 : G_DROP + f * 8 + 8, :] = jnp.where(first, out[0], out[1])
    g_ref[G_LIST : G_LIST + 8, :] = jnp.broadcast_to(small_ref[...], (8, 128))


def pack_gx_kernel(
    q_ref, t_ref, sz_ref, wt_ref, dn_ref, ox_ref, oy_ref, pm_ref, list_ref, south_ref, north_ref,
    east_ref, west_ref,
):
    lane16 = lanes_of((16, 128))
    ext = []
    for a in range(2):
        rows = slice(G_AIR + 16 * a, G_AIR + 16 * a + 16)
        ext.append(jnp.where(lane16 < 64, north_ref[rows, :], south_ref[rows, :]))
    lane = lanes_of((8, 128))
    small = jnp.where(
        (lane < 48) | ((lane >= 96) & (lane < 112)),
        south_ref[G_LIST : G_LIST + 8, :],
        north_ref[G_LIST : G_LIST + 8, :],
    )
    corners = []
    for f in range(FIELDS):
        rows = slice(G_DROP + 8 * f, G_DROP + 8 * f + 8)
        corners.append(jnp.where(lane < 32, south_ref[rows, :], north_ref[rows, :]))
    refs = (sz_ref, wt_ref, dn_ref, ox_ref, oy_ref, pm_ref)
    for side, (out_ref, i) in enumerate(((east_ref, 7), (west_ref, 0))):
        for f, ref in enumerate(refs):
            face = ref[pl.ds(i, 16, stride=8), :]
            if f == 5:
                face = face.astype(F32)
            out_ref[X_DROP + 16 * f : X_DROP + 16 * f + 16, :] = face
            out_ref[X_CORNER + 8 * f : X_CORNER + 8 * f + 8, :] = corners[f]
        out_ref[X_AIR : X_AIR + 16, :] = q_ref[...]
        out_ref[X_AIR + 16 : X_AIR + 32, :] = t_ref[...]
        out_ref[X_EXT : X_EXT + 16, :] = ext[0]
        out_ref[X_EXT + 16 : X_EXT + 32, :] = ext[1]
        out_ref[X_LIST : X_LIST + 8, :] = list_ref[side].astype(F32)
        out_ref[X_SMALL : X_SMALL + 8, :] = small


def departed_kernel(list_ref, small_ref, mask_ref):
    entries = jnp.concatenate(
        [list_ref[0, r : r + 1, :] for r in range(8)]
        + [list_ref[1, r : r + 1, :] for r in range(8)]
        + [small_ref[...].astype(I32)],
        1,
    )
    width = entries.shape[1]
    index = rows_of((128, width))
    row = jnp.broadcast_to(entries >> 7, (128, width))
    column = jnp.broadcast_to(entries & 127, (128, width))
    one_row = jnp.where(row == index, 1.0, 0.0).astype(jnp.bfloat16)
    one_column = jnp.where(column == index, 1.0, 0.0).astype(jnp.bfloat16)
    mask_ref[...] = lax.dot_general(
        one_row, one_column, (((1,), (1,)), ((), ())), preferred_element_type=F32
    )


def kernel_weights(offset):
    return (
        jnp.maximum(0.5 - offset, 0.0),
        1.0 - jnp.abs(offset - 0.5),
        jnp.maximum(offset - 0.5, 0.0),
    )


def cube_root(x):
    y = jnp.exp(jnp.log(x) * (1.0 / 3.0))
    return y - (y * y * y - x) / (3.0 * y * y)


def grow(size, dry, forcing):
    initial = size * size
    lowest = dry * dry
    solute = KAPPA_SOLUTE * lowest * dry
    wetted = initial
    for _ in range(NEWTON):
        root = lax.rsqrt(wetted)
        inverse_square = root * root
        inverse = inverse_square * root
        residue = wetted - initial - GROWTH_STEP * (forcing + solute * inverse)
        slope = 1.0 + (1.5 * GROWTH_STEP) * solute * (inverse * inverse_square)
        wetted = jnp.maximum(wetted - residue / slope, lowest)
    return wetted


def pick(values, bits):
    low, mid, high = bits
    a = [jnp.where(low, values[2 * n + 1], values[2 * n]) for n in range(4)]
    b = [jnp.where(mid, a[2 * n + 1], a[2 * n]) for n in range(2)]
    return jnp.where(high, b[1], b[0])


def coalesce(grown, mult, order):
    bits = [((o & 1) == 1, (o & 2) == 2, (o & 4) == 4) for o in order]
    new_radius, new_mult = [], []
    for pair in range(SD // 2):
        p, q = bits[2 * pair], bits[2 * pair + 1]
        r1, r2 = pick(grown, p), pick(grown, q)
        m1, m2 = pick(mult, p), pick(mult, q)
        big = m1 >= m2
        hr, lr = jnp.where(big, r1, r2), jnp.where(big, r2, r1)
        hm, lm = jnp.where(big, m1, m2), jnp.where(big, m2, m1)
        total = r1 + r2
        rate = COLLIDE_RATE * hm * total * total * jnp.abs(r1 * r1 - r2 * r2)
        chance = 1.0 - jnp.exp(-rate)
        merged = cube_root(lr * lr * lr + chance * hr * hr * hr)
        reduced = hm - chance * lm
        new_radius += [jnp.where(big, hr, merged), jnp.where(big, merged, hr)]
        new_mult += [jnp.where(big, reduced, lm), jnp.where(big, lm, reduced)]
    out_radius, out_mult = [], []
    for target in range(SD):
        r, m = new_radius[0], new_mult[0]
        for position in range(1, SD):
            hit = order[position] == target
            r = jnp.where(hit, new_radius[position], r)
            m = jnp.where(hit, new_mult[position], m)
        out_radius.append(r)
        out_mult.append(m)
    return out_radius, out_mult


def shift(x, amount, axis):
    return pltpu.roll(x, amount % x.shape[axis], axis)


def droplets(windows, size, mult, dry, east, north, order):
    deposit = [[None] * 3 for _ in range(3)]
    grown = []
    for k in range(SD):
        wx, wy = kernel_weights(east[k]), kernel_weights(north[k])
        forcing = -(CURVATURE / size[k])
        for a in range(3):
            line = wy[0] * windows[a][0] + wy[1] * windows[a][1] + wy[2] * windows[a][2]
            forcing = forcing + wx[a] * line
        wetted = grow(size[k], dry[k], forcing)
        radius = jnp.sqrt(wetted)
        condensed = mult[k] * (wetted * radius - size[k] * size[k] * size[k])
        for a in range(3):
            part = wx[a] * condensed
            for b in range(3):
                term = part * wy[b]
                deposit[a][b] = term if k == 0 else deposit[a][b] + term
        grown.append(radius)
    radius, coalesced = coalesce(grown, mult, order)
    return radius, coalesced, deposit


def physics_kernel(
    q_ref, t_ref, sz_ref, wt_ref, dn_ref, ox_ref, oy_ref, pm_ref, mask_ref,
    south_ref, north_ref, west_ref, east_ref,
    moist_ref, warm_ref, size_ref, mult_ref, record_ref, box_ref,
    halo_ref, table_ref,
):
    lane16 = lanes_of((16, 128))
    lane = lanes_of((8, 128))
    row8 = rows_of((8, 128))
    slot = lane % 16

    air = []
    for a, own_ref in enumerate((q_ref, t_ref)):
        g_rows = slice(G_AIR + 16 * a, G_AIR + 16 * a + 16)
        ext = jnp.where(lane16 < 64, north_ref[g_rows, :], south_ref[g_rows, :])
        levels = []
        for l in range(2):
            rows = []
            for ref in (west_ref, None, east_ref):
                if ref is None:
                    main = own_ref[8 * l : 8 * l + 8, :]
                    side = ext[8 * l : 8 * l + 8, :]
                else:
                    base = 16 * a + 8 * l
                    main = ref[X_AIR + base : X_AIR + base + 8, :]
                    side = ref[X_EXT + base : X_EXT + base + 8, :]
                rows.append(jnp.concatenate([main, side], 1))
            levels.append(jnp.concatenate(rows, 0))
        air.append(levels)
    mixed = []
    for a in range(2):
        both = []
        for l in range(2):
            x = air[a][l]
            other = air[a][1 - l]
            across = (
                shift(x, 1, 0) + shift(x, -1, 0) + shift(x, 1, 1) + shift(x, -1, 1) - 4.0 * x
            )
            both.append(x + MIX_HORIZONTAL * across + MIX_VERTICAL * (other + x - 2.0 * x))
        mixed.append(both)
    moved = []
    turned = []
    for l in range(2):
        vapour, warm = mixed[0][l], mixed[1][l]
        most = EXCESS_FACTOR * jnp.exp(17.27 * (warm - 273.15) / (warm - 35.86))
        humid = vapour / most - 1.0
        columns = [shift(humid, 1, 1), humid, shift(humid, -1, 1)]
        moved.append([[shift(c[:, :128], 1, 0) for c in columns],
                      [c[:, :128] for c in columns],
                      [shift(c[:, :128], -1, 0) for c in columns]])
        ahead = shift(humid, 2, 1)
        tall = lanes_of((24, 128))
        near = jnp.where(tall < 8, ahead[:, :128], shift(ahead[:, 128:], 8, 1))
        turned.append(near[4:20, :])
    strip = jnp.concatenate(turned + turned + turned + turned, 0)
    strip = jnp.transpose(strip)
    lane1 = lanes_of((1, 128))
    rim = []
    for b in range(3):
        line = jnp.where(lane1 < 32, strip[b : b + 1, :], strip[b + 9 : b + 10, :])
        rim.append([shift(line, 1, 1), line, shift(line, -1, 1)])

    beyond = []
    for f in range(FIELDS):
        c_rows = slice(X_CORNER + 8 * f, X_CORNER + 8 * f + 8)
        g_rows = slice(G_DROP + 8 * f, G_DROP + 8 * f + 8)
        own = jnp.where(lane < 32, south_ref[g_rows, :], north_ref[g_rows, :])
        line = jnp.where(
            slot == 3,
            shift(west_ref[c_rows, :], -8, 1),
            jnp.where(slot == 12, shift(east_ref[c_rows, :], 8, 1), own),
        )
        line = jnp.where((lane < 64) & (slot >= 3) & (slot <= 12), line, 0.0 if f == 5 else 0.5)
        beyond.append(line)
        for l in range(2):
            base = X_DROP + 16 * f + l
            halo_ref[f, pl.ds(l, 8, stride=8), :] = west_ref[pl.ds(base, 8, stride=2), :]
            halo_ref[f, pl.ds(2 + l, 8, stride=8), :] = east_ref[pl.ds(base, 8, stride=2), :]
        for r in range(4, 8):
            halo_ref[f, pl.ds(r, 8, stride=8), :] = line

    deposits = []
    for l in range(2):
        windows = [[moved[l][a][b][8:16, :] for b in range(3)] for a in range(3)]
        tiles = [
            [ref[k * 16 + 8 * l : k * 16 + 8 * l + 8, :] for k in range(SD)]
            for ref in (sz_ref, wt_ref, dn_ref, ox_ref, oy_ref, pm_ref)
        ]
        radius, coalesced, deposit = droplets(windows, *tiles)
        for k in range(SD):
            rows = slice(k * 16 + 8 * l, k * 16 + 8 * l + 8)
            size_ref[rows, :] = radius[k]
            mult_ref[rows, :] = jnp.where(mask_ref[rows, :] > 0.5, 0.0, coalesced[k])
        deposits.append(deposit)
    windows = []
    for a in range(3):
        line = []
        for b in range(3):
            line.append(jnp.concatenate(
                [moved[0][a][b][7:8, :], moved[1][a][b][7:8, :],
                 moved[0][a][b][16:17, :], moved[1][a][b][16:17, :]] + [rim[b][a]] * 4, 0))
        windows.append(line)
    tiles = [[halo_ref[f, 8 * k : 8 * k + 8, :] for k in range(SD)] for f in range(5)]
    order = [halo_ref[5, 8 * k : 8 * k + 8, :].astype(I32) for k in range(SD)]
    halo_radius, halo_mult, outer = droplets(windows, *tiles, order)
    for k in range(SD):
        table_ref[0, 8 * k : 8 * k + 8, :] = halo_radius[k]
        table_ref[1, 8 * k : 8 * k + 8, :] = halo_mult[k]

    def along_y(d, a):
        return (
            d[a][1]
            + jnp.where(lane == 0, 0.0, shift(d[a][2], 1, 1))
            + jnp.where(lane == 127, 0.0, shift(d[a][0], -1, 1))
        )

    from_west = along_y(outer, 2)
    from_east = along_y(outer, 0)
    rim_line = [jnp.where(lane1 < 32, outer[a][2][4:5, :], outer[a][0][4:5, :]) for a in range(3)]
    rim_line = shift(rim_line[2], 1, 1) + rim_line[1] + shift(rim_line[0], -1, 1)
    rim_line = jnp.broadcast_to(rim_line, (8, 128))
    for l in range(2):
        own = [along_y(deposits[l], a) for a in range(3)]
        west_row = jnp.broadcast_to(from_west[l : l + 1, :], (8, 128))
        east_row = jnp.broadcast_to(from_east[2 + l : 3 + l, :], (8, 128))
        source = (
            own[1]
            + jnp.where(row8 == 0, west_row, shift(own[2], 1, 0))
            + jnp.where(row8 == 7, east_row, shift(own[0], -1, 0))
        )
        for side, j in enumerate((0, 127)):
            wanted = lane == side * 32 + l * 16 + 4 + row8
            column = jnp.sum(jnp.where(wanted, rim_line, 0.0), axis=1, keepdims=True)
            source = source + jnp.where(lane == j, column, 0.0)
        rows = slice(8 * l, 8 * l + 8)
        moist_ref[rows, :] = mixed[0][l][8:16, :128] - VAPOUR_PER_SOURCE * source
        warm_ref[rows, :] = mixed[1][l][8:16, :128] + WARMING_FACTOR * source

    for side, (ref, dx) in enumerate(((west_ref, 1), (east_ref, -1))):
        entry = ref[X_LIST : X_LIST + 8, :].astype(I32)
        live = entry >= 0
        column = entry & 127
        group = entry >> 10
        picked = [jnp.zeros((8, 128), F32) for _ in range(5)]
        for k in range(SD):
            for l in range(2):
                here = live & (group == 2 * k + l)
                r = 8 * k + 2 * side + l
                for n in range(5):
                    src = table_ref if n < 2 else halo_ref
                    line = jnp.broadcast_to(src[n, r : r + 1, :], (8, 128))
                    got = jnp.take_along_axis(line, column, axis=1)
                    picked[n] = jnp.where(here, got, picked[n])
        box = (((entry >> 10) & 1) * 8 + (((entry >> 7) + dx) & 7)) * 128 + column
        box = jnp.where(live, box, -1)
        for c in range(8):
            at = side * 1024 + c * 128
            for n in range(5):
                record_ref[n, 0:1, at : at + 128] = picked[n][c : c + 1, :]
            box_ref[0:1, at : at + 128] = box[c : c + 1, :]

    own_small = jnp.where(
        (lane < 48) | ((lane >= 96) & (lane < 112)),
        south_ref[G_LIST : G_LIST + 8, :],
        north_ref[G_LIST : G_LIST + 8, :],
    )
    diagonal = lane >= 96
    by_west = diagonal & (lane % 16 < 8)
    entry = jnp.where(
        by_west,
        west_ref[X_SMALL : X_SMALL + 8, :],
        jnp.where(diagonal, east_ref[X_SMALL : X_SMALL + 8, :], own_small),
    ).astype(I32)
    live = entry >= 0
    north_side = ((lane >= 48) & (lane < 96)) | (lane >= 112)
    column = entry & 127
    i = (entry >> 7) & 7
    level = (entry >> 10) & 1
    place = i + 4 + jnp.where(diagonal, jnp.where(by_west, -8, 8), 0)
    at = (jnp.where(north_side, 32, 0) + level * 16 + place) & 127
    mine = live & ((entry >> 11) == row8)
    dx = jnp.where(diagonal, jnp.where(by_west, 1, -1), 0)
    dy = jnp.where(north_side, -1, 1)
    box = (level * 8 + ((i + dx) & 7)) * 128 + ((column + dy) & 127)
    box_ref[0:1, 2048:2176] = jnp.where(live, box, -1)[0:1, :]
    for n in range(5):
        if n < 2:
            table = table_ref[n, pl.ds(4, 8, stride=8), :]
        else:
            table = beyond[n]
        got = jnp.take_along_axis(table, at, axis=1)
        line = jnp.sum(jnp.where(mine, got, 0.0), axis=0, keepdims=True)
        record_ref[n, 0:1, 2048:2176] = line


def whole(count):
    return [pl.BlockSpec(memory_space=pltpu.VMEM)] * count


def call(kernel, outs, args, scratch=(), flops=1 << 20):
    return pl.pallas_call(
        kernel,
        out_shape=outs,
        in_specs=whole(len(args)),
        out_specs=jax.tree.map(lambda _: pl.BlockSpec(memory_space=pltpu.VMEM), outs),
        scratch_shapes=list(scratch),
        cost_estimate=pl.CostEstimate(flops=flops, bytes_accessed=1 << 18, transcendentals=0),
    )(*args)


def ring(axis, step):
    count = lax.axis_size(axis)
    return [(i, (i + step) % count) for i in range(count)]


def per_device(
    moisture_ratio,
    kelvin_warmth,
    droplet_size_micron,
    weighting_factor,
    dry_nucleus_size,
    fractional_offset_east,
    fractional_offset_north,
    encounter_permutation,
    departing_eastwest_lists,
    departing_northsouth_lists,
    departing_diagonal_lists,
):
    def f32(*shape):
        return jax.ShapeDtypeStruct(shape, F32)

    air = (moisture_ratio.reshape(16, 128), kelvin_warmth.reshape(16, 128))
    drops = tuple(
        x.reshape(128, 128)
        for x in (
            droplet_size_micron,
            weighting_factor,
            dry_nucleus_size,
            fractional_offset_east,
            fractional_offset_north,
            encounter_permutation,
        )
    )
    long_lists = departing_eastwest_lists.reshape(2, 8, 128)
    corner = departing_diagonal_lists[0]
    small = (
        jnp.concatenate(
            [departing_northsouth_lists.reshape(-1), corner[0], corner[2], corner[1], corner[3]]
        )
        .astype(F32)
        .reshape(1, 128)
    )
    to_gy = call(pack_gy_kernel, f32(G_ROWS, 128), (*air, *drops, small))
    from_south = lax.ppermute(to_gy, "gy", ring("gy", 1))
    from_north = lax.ppermute(to_gy, "gy", ring("gy", -1))
    to_east, to_west = call(
        pack_gx_kernel,
        (f32(X_ROWS, 128), f32(X_ROWS, 128)),
        (*air, *drops, long_lists, from_south, from_north),
    )
    from_west = lax.ppermute(to_east, "gx", ring("gx", 1))
    from_east = lax.ppermute(to_west, "gx", ring("gx", -1))
    departed = call(departed_kernel, f32(128, 128), (long_lists, small))
    moist, warm, size, mult, records, box = call(
        physics_kernel,
        (
            f32(16, 128),
            f32(16, 128),
            f32(128, 128),
            f32(128, 128),
            f32(5, 1, 2176),
            jax.ShapeDtypeStruct((1, 2176), I32),
        ),
        (*air, *drops, departed, from_south, from_north, from_west, from_east),
        scratch=(pltpu.VMEM((FIELDS, 64, 128), F32), pltpu.VMEM((2, 64, 128), F32)),
    )
    return (
        moist.reshape(moisture_ratio.shape),
        warm.reshape(kelvin_warmth.shape),
        size.reshape(droplet_size_micron.shape),
        mult.reshape(weighting_factor.shape),
        records,
        box,
    )


def solution(mesh):
    cells = P(None, "gx", "gy")
    drop = P(None, None, "gx", "gy")
    lists = P("gx", None, "gy")
    return jax.shard_map(
        per_device,
        mesh=mesh,
        in_specs=(cells,) * 2 + (drop,) * 6 + (lists,) * 3,
        out_specs=(cells, cells, drop, drop, P(None, "gx", "gy"), P("gx", "gy")),
        check_vma=False,
    )
```

```python
import jax
import jax.numpy as jnp
from jax import lax
from jax.experimental import pallas as pl
from jax.experimental.pallas import tpu as pltpu
from jax.sharding import PartitionSpec as P


NEWTON = 4
MIX_HORIZONTAL = 0.2
MIX_VERTICAL = 0.05
EXCESS_FACTOR = 4.2222
CURVATURE = 0.0012
KAPPA_SOLUTE = 0.6
GROWTH_STEP = 200.0
COLLIDE_RATE = 4e-07
VAPOUR_PER_SOURCE = 0.001
WARMING_FACTOR = 0.00249

F32 = jnp.float32
I32 = jnp.int32
SD = 8
FIELDS = 6

G_LIST = 8 * FIELDS
G_ROWS = G_LIST + 8
X_AIR = 16 * FIELDS
X_CORNER = X_AIR + 16
X_LIST = X_CORNER + 8
X_ROWS = X_LIST + 8


def lanes_of(shape):
    return lax.broadcasted_iota(I32, shape, len(shape) - 1)


def shift(x, amount, axis):
    return pltpu.roll(x, amount % x.shape[axis], axis)


def rows_of(shape):
    return lax.broadcasted_iota(I32, shape, len(shape) - 2)


def pack_gy_kernel(*refs):
    given, kept = refs[:11], refs[11:20]
    g_ref, side_ref, corner_ref, line_ref, sems = refs[20:]
    copies = [
        pltpu.make_async_copy(source, target, sems.at[n])
        for n, (source, target) in enumerate(zip(given, (*kept, side_ref, corner_ref)))
    ]
    for n in (9, 10, 0, 1, 2, 3, 4, 5, 6, 7, 8):
        copies[n].start()
    copies[9].wait()
    copies[10].wait()
    line_ref[0:2, 0:48] = side_ref[0].astype(F32)
    line_ref[2:6, 0:8] = corner_ref[0].astype(F32)
    small = line_ref[0:1, :]
    lane1 = lanes_of((1, 128))
    for row, start in ((1, 48), (2, 96), (4, 104), (3, 112), (5, 120)):
        small = jnp.where(lane1 < start, small, pltpu.roll(line_ref[row : row + 1, :], start, 1))
    g_ref[G_LIST:G_ROWS, :] = jnp.broadcast_to(small, (8, 128))
    copies[0].wait()
    copies[1].wait()
    lane = lanes_of((8, 128))
    first = lane < 32
    low_level = lane % 32 < 16
    for f in range(FIELDS):
        copies[2 + f].wait()
        ref = kept[2 + f]
        parts = [ref[k * 16 : k * 16 + 16, :] for k in range(SD - 1, -1, -1)]
        block = jnp.concatenate(parts, 0)
        if f == 5:
            block = block.astype(F32)
        turned = jnp.transpose(block)
        out = []
        for base, row in ((0, 127), (32, 0)):
            line = jnp.broadcast_to(turned[row : row + 1, :], (8, 128))
            line = pltpu.roll(line, 16, 1, stride=16, stride_axis=0)
            lev0 = pltpu.roll(line, base + 4, 1)
            lev1 = pltpu.roll(line, base + 12, 1)
            out.append(jnp.where(low_level, lev0, lev1))
        block = jnp.where(first, out[0], out[1])
        if f < 4:
            air = kept[f // 2][8 * (f % 2) : 8 * (f % 2) + 8, :]
            block = jnp.where(lane < 64, block, pltpu.roll(air, 67, 1))
        g_ref[f * 8 : f * 8 + 8, :] = block
    copies[8].wait()


def pack_gx_kernel(
    q_ref, t_ref, sz_ref, wt_ref, dn_ref, ox_ref, oy_ref, pm_ref, list_ref, near_ref, far_ref,
    east_ref, west_ref, rim_ref,
):
    even = lax.axis_index("gy") % 2 == 0
    lane = lanes_of((8, 128))
    slot = lane % 16
    from_near = (((lane >= 32) & (lane < 64)) | (lane >= 67)) == even
    blocks = []
    for f in range(FIELDS):
        rows = slice(8 * f, 8 * f + 8)
        merged = jnp.where(from_near, near_ref[rows, :], far_ref[rows, :])
        rim_ref[rows, :] = merged
        blocks.append(merged)
    from_near = (((lane >= 48) & (lane < 96)) | (lane >= 112)) == even
    small = jnp.where(from_near, near_ref[G_LIST:G_ROWS, :], far_ref[G_LIST:G_ROWS, :])
    rim_ref[G_LIST:G_ROWS, :] = small
    drops = (sz_ref, wt_ref, dn_ref, ox_ref, oy_ref, pm_ref)
    for side, (out_ref, i, row) in enumerate(((east_ref, 7, 5), (west_ref, 0, 0))):
        for f, ref in enumerate(drops):
            face = ref[pl.ds(i, 16, stride=8), :]
            if f == 5:
                face = face.astype(F32)
            out_ref[16 * f : 16 * f + 16, :] = face
        for g in range(4):
            ref = (q_ref, t_ref)[g // 2]
            at = 8 * (g % 2) + row
            out_ref[X_AIR + 3 * g : X_AIR + 3 * g + 3, :] = ref[at : at + 3, :]
        out_ref[X_AIR + 12 : X_AIR + 16, :] = jnp.zeros((4, 128), F32)
        corner = small
        for g in range(4):
            here = (lane >= 64 + 8 * g) & (lane < 72 + 8 * g)
            corner = jnp.where(here, shift(blocks[g], 8 * g, 1), corner)
        for f in range(FIELDS):
            here = (lane < 64) & (slot == f)
            corner = jnp.where(here, shift(blocks[f], f - 4 - i, 1), corner)
        out_ref[X_CORNER : X_CORNER + 8, :] = corner
        for c in range(8):
            piece = list_ref[0, side : side + 1, 128 * c : 128 * c + 128]
            out_ref[X_LIST + c : X_LIST + c + 1, :] = piece.astype(F32)


def one_hot(values, rows):
    shape = (rows, values.shape[1])
    hit = jnp.broadcast_to(values, shape) == rows_of(shape)
    return jnp.where(hit, 1.0, 0.0).astype(jnp.bfloat16)


def counts(rows, columns):
    return lax.dot_general(rows, columns, (((1,), (1,)), ((), ())), preferred_element_type=F32)


def departed_kernel(list_ref, g_ref, mask_ref):
    entry = g_ref[G_LIST : G_LIST + 1, :].astype(I32)
    mask_ref[...] = counts(one_hot(entry >> 7, 128), one_hot(entry & 127, 128))
    for side, i in ((0, 7), (1, 0)):
        entry = list_ref[0, side : side + 1, :]
        found = counts(one_hot(entry >> 10, 16), one_hot(entry & 127, 128))
        rows = pl.ds(i, 16, stride=8)
        mask_ref[rows, :] = mask_ref[rows, :] + found


def kernel_weights(offset):
    return (
        jnp.maximum(0.5 - offset, 0.0),
        1.0 - jnp.abs(offset - 0.5),
        jnp.maximum(offset - 0.5, 0.0),
    )


def cube_root(x):
    y = jnp.exp(jnp.log(x) * (1.0 / 3.0))
    return y - (y * y * y - x) / (3.0 * y * y)


def grow(size, dry, forcing):
    initial = size * size
    lowest = dry * dry
    solute = KAPPA_SOLUTE * lowest * dry
    wetted = initial
    for _ in range(NEWTON):
        root = lax.rsqrt(wetted)
        inverse_square = root * root
        inverse = inverse_square * root
        residue = wetted - initial - GROWTH_STEP * (forcing + solute * inverse)
        slope = 1.0 + (1.5 * GROWTH_STEP) * solute * (inverse * inverse_square)
        wetted = jnp.maximum(wetted - residue / slope, lowest)
    return wetted


def pick(values, bits):
    low, mid, high = bits
    a = [jnp.where(low, values[2 * n + 1], values[2 * n]) for n in range(4)]
    b = [jnp.where(mid, a[2 * n + 1], a[2 * n]) for n in range(2)]
    return jnp.where(high, b[1], b[0])


def coalesce(grown, mult, order):
    bits = [((o & 1) == 1, (o & 2) == 2, (o & 4) == 4) for o in order]
    new_radius, new_mult = [], []
    for pair in range(SD // 2):
        p, q = bits[2 * pair], bits[2 * pair + 1]
        r1, r2 = pick(grown, p), pick(grown, q)
        m1, m2 = pick(mult, p), pick(mult, q)
        big = m1 >= m2
        hr, lr = jnp.where(big, r1, r2), jnp.where(big, r2, r1)
        hm, lm = jnp.where(big, m1, m2), jnp.where(big, m2, m1)
        total = r1 + r2
        rate = COLLIDE_RATE * hm * total * total * jnp.abs(r1 * r1 - r2 * r2)
        chance = 1.0 - jnp.exp(-rate)
        merged = cube_root(lr * lr * lr + chance * hr * hr * hr)
        reduced = hm - chance * lm
        new_radius += [jnp.where(big, hr, merged), jnp.where(big, merged, hr)]
        new_mult += [jnp.where(big, reduced, lm), jnp.where(big, lm, reduced)]
    out_radius, out_mult = [], []
    for target in range(SD):
        r, m = new_radius[0], new_mult[0]
        for position in range(1, SD):
            hit = order[position] == target
            r = jnp.where(hit, new_radius[position], r)
            m = jnp.where(hit, new_mult[position], m)
        out_radius.append(r)
        out_mult.append(m)
    return out_radius, out_mult


def droplets(windows, size, mult, dry, east, north, order):
    deposit = [[None] * 3 for _ in range(3)]
    grown = []
    for k in range(SD):
        wx, wy = kernel_weights(east[k]), kernel_weights(north[k])
        forcing = -(CURVATURE / size[k])
        for a in range(3):
            line = wy[0] * windows[a][0] + wy[1] * windows[a][1] + wy[2] * windows[a][2]
            forcing = forcing + wx[a] * line
        wetted = grow(size[k], dry[k], forcing)
        radius = jnp.sqrt(wetted)
        condensed = mult[k] * (wetted * radius - size[k] * size[k] * size[k])
        for a in range(3):
            part = wx[a] * condensed
            for b in range(3):
                term = part * wy[b]
                deposit[a][b] = term if k == 0 else deposit[a][b] + term
        grown.append(radius)
    radius, coalesced = coalesce(grown, mult, order)
    return radius, coalesced, deposit


def physics_kernel(
    q_ref, t_ref, sz_ref, wt_ref, dn_ref, ox_ref, oy_ref, pm_ref, mask_ref,
    rim_ref, west_ref, east_ref,
    moist_ref, warm_ref, size_ref, mult_ref, record_ref, box_ref,
    halo_ref, table_ref, air_ref,
):
    lane = lanes_of((8, 128))
    row8 = rows_of((8, 128))
    slot = lane % 16

    air = []
    for a, own_ref in enumerate((q_ref, t_ref)):
        levels = []
        for l in range(2):
            g = 2 * a + l
            row = X_AIR + 3 * g
            air_ref[g, 8:16, :128] = own_ref[8 * l : 8 * l + 8, :]
            air_ref[g, 8:16, 128:] = shift(rim_ref[8 * g : 8 * g + 8, :], -67, 1)
            air_ref[g, 5:8, :128] = west_ref[row : row + 3, :]
            air_ref[g, 0:8, 128:] = shift(west_ref[X_CORNER : X_CORNER + 8, :], -67 - 8 * g, 1)
            air_ref[g, 16:19, :128] = east_ref[row : row + 3, :]
            air_ref[g, 16:24, 128:] = shift(east_ref[X_CORNER : X_CORNER + 8, :], -67 - 8 * g, 1)
            levels.append(air_ref[g])
        air.append(levels)
    mixed = []
    for a in range(2):
        both = []
        for l in range(2):
            x = air[a][l]
            other = air[a][1 - l]
            across = (
                shift(x, 1, 0) + shift(x, -1, 0) + shift(x, 1, 1) + shift(x, -1, 1) - 4.0 * x
            )
            both.append(x + MIX_HORIZONTAL * across + MIX_VERTICAL * (other + x - 2.0 * x))
        mixed.append(both)
    moved = []
    turned = []
    for l in range(2):
        vapour, warm = mixed[0][l], mixed[1][l]
        most = EXCESS_FACTOR * jnp.exp(17.27 * (warm - 273.15) / (warm - 35.86))
        humid = vapour / most - 1.0
        columns = [shift(humid, 1, 1), humid, shift(humid, -1, 1)]
        moved.append([[shift(c[:, :128], 1, 0) for c in columns],
                      [c[:, :128] for c in columns],
                      [shift(c[:, :128], -1, 0) for c in columns]])
        ahead = shift(humid, 2, 1)
        tall = lanes_of((24, 128))
        near = jnp.where(tall < 8, ahead[:, :128], shift(ahead[:, 128:], 8, 1))
        turned.append(near[4:20, :])
    strip = jnp.concatenate(turned + turned + turned + turned, 0)
    strip = jnp.transpose(strip)
    lane1 = lanes_of((1, 128))
    rim = []
    for b in range(3):
        line = jnp.where(lane1 < 32, strip[b : b + 1, :], strip[b + 9 : b + 10, :])
        rim.append([shift(line, 1, 1), line, shift(line, -1, 1)])

    beyond = []
    for f in range(FIELDS):
        line = jnp.where(
            slot == 3,
            shift(west_ref[X_CORNER : X_CORNER + 8, :], 3 - f, 1),
            jnp.where(
                slot == 12,
                shift(east_ref[X_CORNER : X_CORNER + 8, :], 12 - f, 1),
                rim_ref[8 * f : 8 * f + 8, :],
            ),
        )
        line = jnp.where((lane < 64) & (slot >= 3) & (slot <= 12), line, 0.0 if f == 5 else 0.5)
        beyond.append(line)
        for l in range(2):
            base = 16 * f + l
            halo_ref[f, pl.ds(l, 8, stride=8), :] = west_ref[pl.ds(base, 8, stride=2), :]
            halo_ref[f, pl.ds(2 + l, 8, stride=8), :] = east_ref[pl.ds(base, 8, stride=2), :]
        for r in range(4, 8):
            halo_ref[f, pl.ds(r, 8, stride=8), :] = line

    deposits = []
    for l in range(2):
        windows = [[moved[l][a][b][8:16, :] for b in range(3)] for a in range(3)]
        tiles = [
            [ref[k * 16 + 8 * l : k * 16 + 8 * l + 8, :] for k in range(SD)]
            for ref in (sz_ref, wt_ref, dn_ref, ox_ref, oy_ref, pm_ref)
        ]
        radius, coalesced, deposit = droplets(windows, *tiles)
        for k in range(SD):
            rows = slice(k * 16 + 8 * l, k * 16 + 8 * l + 8)
            size_ref[rows, :] = radius[k]
            mult_ref[rows, :] = jnp.where(mask_ref[rows, :] > 0.5, 0.0, coalesced[k])
        deposits.append(deposit)
    windows = []
    for a in range(3):
        line = []
        for b in range(3):
            line.append(jnp.concatenate(
                [moved[0][a][b][7:8, :], moved[1][a][b][7:8, :],
                 moved[0][a][b][16:17, :], moved[1][a][b][16:17, :]] + [rim[b][a]] * 4, 0))
        windows.append(line)
    tiles = [[halo_ref[f, 8 * k : 8 * k + 8, :] for k in range(SD)] for f in range(5)]
    order = [halo_ref[5, 8 * k : 8 * k + 8, :].astype(I32) for k in range(SD)]
    halo_radius, halo_mult, outer = droplets(windows, *tiles, order)
    for k in range(SD):
        table_ref[0, 8 * k : 8 * k + 8, :] = halo_radius[k]
        table_ref[1, 8 * k : 8 * k + 8, :] = halo_mult[k]

    def along_y(d, a):
        return (
            d[a][1]
            + jnp.where(lane == 0, 0.0, shift(d[a][2], 1, 1))
            + jnp.where(lane == 127, 0.0, shift(d[a][0], -1, 1))
        )

    from_west = along_y(outer, 2)
    from_east = along_y(outer, 0)
    rim_line = [jnp.where(lane1 < 32, outer[a][2][4:5, :], outer[a][0][4:5, :]) for a in range(3)]
    rim_line = shift(rim_line[2], 1, 1) + rim_line[1] + shift(rim_line[0], -1, 1)
    rim_line = jnp.broadcast_to(rim_line, (8, 128))
    for l in range(2):
        own = [along_y(deposits[l], a) for a in range(3)]
        west_row = jnp.broadcast_to(from_west[l : l + 1, :], (8, 128))
        east_row = jnp.broadcast_to(from_east[2 + l : 3 + l, :], (8, 128))
        source = (
            own[1]
            + jnp.where(row8 == 0, west_row, shift(own[2], 1, 0))
            + jnp.where(row8 == 7, east_row, shift(own[0], -1, 0))
        )
        for side, j in enumerate((0, 127)):
            wanted = lane == side * 32 + l * 16 + 4 + row8
            column = jnp.sum(jnp.where(wanted, rim_line, 0.0), axis=1, keepdims=True)
            source = source + jnp.where(lane == j, column, 0.0)
        rows = slice(8 * l, 8 * l + 8)
        moist_ref[rows, :] = mixed[0][l][8:16, :128] - VAPOUR_PER_SOURCE * source
        warm_ref[rows, :] = mixed[1][l][8:16, :128] + WARMING_FACTOR * source

    for side, (ref, dx) in enumerate(((west_ref, 1), (east_ref, -1))):
        entry = ref[X_LIST : X_LIST + 8, :].astype(I32)
        live = entry >= 0
        column = entry & 127
        group = entry >> 10
        picked = [jnp.zeros((8, 128), F32) for _ in range(5)]
        for k in range(SD):
            for l in range(2):
                here = live & (group == 2 * k + l)
                r = 8 * k + 2 * side + l
                for n in range(5):
                    src = table_ref if n < 2 else halo_ref
                    line = jnp.broadcast_to(src[n, r : r + 1, :], (8, 128))
                    got = jnp.take_along_axis(line, column, axis=1)
                    picked[n] = jnp.where(here, got, picked[n])
        box = (((entry >> 10) & 1) * 8 + (((entry >> 7) + dx) & 7)) * 128 + column
        box = jnp.where(live, box, -1)
        for c in range(8):
            at = side * 1024 + c * 128
            for n in range(5):
                record_ref[n, 0:1, at : at + 128] = picked[n][c : c + 1, :]
            box_ref[0:1, at : at + 128] = box[c : c + 1, :]

    diagonal = lane >= 96
    by_west = diagonal & (lane % 16 < 8)
    entry = jnp.where(
        by_west,
        west_ref[X_CORNER : X_CORNER + 8, :],
        jnp.where(diagonal, east_ref[X_CORNER : X_CORNER + 8, :], rim_ref[G_LIST:G_ROWS, :]),
    ).astype(I32)
    live = entry >= 0
    north_side = ((lane >= 48) & (lane < 96)) | (lane >= 112)
    column = entry & 127
    i = (entry >> 7) & 7
    level = (entry >> 10) & 1
    place = i + 4 + jnp.where(diagonal, jnp.where(by_west, -8, 8), 0)
    at = (jnp.where(north_side, 32, 0) + level * 16 + place) & 127
    mine = live & ((entry >> 11) == row8)
    dx = jnp.where(diagonal, jnp.where(by_west, 1, -1), 0)
    dy = jnp.where(north_side, -1, 1)
    box = (level * 8 + ((i + dx) & 7)) * 128 + ((column + dy) & 127)
    box_ref[0:1, 2048:2176] = jnp.where(live, box, -1)[0:1, :]
    for n in range(5):
        if n < 2:
            table = table_ref[n, pl.ds(4, 8, stride=8), :]
        else:
            table = beyond[n]
        got = jnp.take_along_axis(table, at, axis=1)
        line = jnp.sum(jnp.where(mine, got, 0.0), axis=0, keepdims=True)
        record_ref[n, 0:1, 2048:2176] = line


def call(kernel, outs, args, scratch=()):
    return pl.pallas_call(
        kernel,
        out_shape=outs,
        in_specs=[pl.BlockSpec(memory_space=pltpu.VMEM)] * len(args),
        out_specs=jax.tree.map(lambda _: pl.BlockSpec(memory_space=pltpu.VMEM), outs),
        scratch_shapes=list(scratch),
        compiler_params=pltpu.CompilerParams(vmem_limit_bytes=8 << 20),
        cost_estimate=pl.CostEstimate(flops=1 << 20, bytes_accessed=1 << 18, transcendentals=0),
    )(*args)


def ring(axis, step):
    count = lax.axis_size(axis)
    return [(i, (i + step) % count) for i in range(count)]


def swaps(axis, first):
    count = lax.axis_size(axis)
    pairs = [(i % count, (i + 1) % count) for i in range(first, count, 2)]
    return pairs + [(target, source) for source, target in pairs]


def per_device(
    moisture_ratio,
    kelvin_warmth,
    droplet_size_micron,
    weighting_factor,
    dry_nucleus_size,
    fractional_offset_east,
    fractional_offset_north,
    encounter_permutation,
    departing_eastwest_lists,
    departing_northsouth_lists,
    departing_diagonal_lists,
):
    def f32(*shape):
        return jax.ShapeDtypeStruct(shape, F32)

    air = (moisture_ratio.reshape(16, 128), kelvin_warmth.reshape(16, 128))
    drops = tuple(
        x.reshape(128, 128)
        for x in (
            droplet_size_micron,
            weighting_factor,
            dry_nucleus_size,
            fractional_offset_east,
            fractional_offset_north,
            encounter_permutation,
        )
    )
    given = (*air, *drops, departing_eastwest_lists)
    short = (departing_northsouth_lists, departing_diagonal_lists)
    *given, east_west, to_gy = pl.pallas_call(
        pack_gy_kernel,
        out_shape=(*(pltpu.VMEM(x.shape, x.dtype) for x in given), pltpu.VMEM((G_ROWS, 128), F32)),
        in_specs=[pl.BlockSpec(memory_space=pltpu.HBM)] * 11,
        out_specs=(pl.BlockSpec(memory_space=pltpu.VMEM),) * 10,
        scratch_shapes=(
            *(pltpu.VMEM(x.shape, x.dtype) for x in short),
            pltpu.VMEM((8, 128), F32),
            pltpu.SemaphoreType.DMA((11,)),
        ),
        compiler_params=pltpu.CompilerParams(vmem_limit_bytes=8 << 20),
        cost_estimate=pl.CostEstimate(flops=1 << 20, bytes_accessed=1 << 18, transcendentals=0),
    )(*(pltpu.with_memory_space_constraint(x, pltpu.HBM) for x in (*given, *short)))
    far = lax.ppermute(to_gy, "gy", swaps("gy", 1))
    near = lax.ppermute(to_gy, "gy", swaps("gy", 0))
    departed = call(departed_kernel, f32(128, 128), (east_west, to_gy))
    to_east, to_west, rim = call(
        pack_gx_kernel,
        (f32(X_ROWS, 128), f32(X_ROWS, 128), f32(G_ROWS, 128)),
        (*given, east_west, near, far),
    )
    from_west = lax.ppermute(to_east, "gx", ring("gx", 1))
    from_east = lax.ppermute(to_west, "gx", ring("gx", -1))
    moist, warm, size, mult, records, box = call(
        physics_kernel,
        (
            f32(16, 128),
            f32(16, 128),
            f32(128, 128),
            f32(128, 128),
            f32(5, 1, 2176),
            jax.ShapeDtypeStruct((1, 2176), I32),
        ),
        (*given, departed, rim, from_west, from_east),
        scratch=(pltpu.VMEM((FIELDS, 64, 128), F32), pltpu.VMEM((2, 64, 128), F32), pltpu.VMEM((4, 24, 256), F32)),
    )
    return (
        moist.reshape(moisture_ratio.shape),
        warm.reshape(kelvin_warmth.shape),
        size.reshape(droplet_size_micron.shape),
        mult.reshape(weighting_factor.shape),
        records,
        box,
    )


def solution(mesh):
    cells = P(None, "gx", "gy")
    drop = P(None, None, "gx", "gy")
    lists = P("gx", None, "gy")
    return jax.shard_map(
        per_device,
        mesh=mesh,
        in_specs=(cells,) * 2 + (drop,) * 6 + (lists,) * 3,
        out_specs=(cells, cells, drop, drop, P(None, "gx", "gy"), P("gx", "gy")),
        check_vma=False,
    )
```

```python
import jax
import jax.numpy as jnp
from jax import lax
from jax.experimental import pallas as pl
from jax.experimental.pallas import tpu as pltpu
from jax.sharding import PartitionSpec as P


NEWTON = 4
MIX_HORIZONTAL = 0.2
MIX_VERTICAL = 0.05
EXCESS_FACTOR = 4.2222
CURVATURE = 0.0012
KAPPA_SOLUTE = 0.6
GROWTH_STEP = 200.0
COLLIDE_RATE = 4e-07
VAPOUR_PER_SOURCE = 0.001
WARMING_FACTOR = 0.00249

F32 = jnp.float32
I32 = jnp.int32
SD = 8
FIELDS = 6

G_LIST = 8 * FIELDS
G_ROWS = G_LIST + 8
X_AIR = 16 * FIELDS
X_CORNER = X_AIR + 16
X_LIST = X_CORNER + 8
X_ROWS = X_LIST + 8


def lanes_of(shape):
    return lax.broadcasted_iota(I32, shape, len(shape) - 1)


def shift(x, amount, axis):
    return pltpu.roll(x, amount % x.shape[axis], axis)


def rows_of(shape):
    return lax.broadcasted_iota(I32, shape, len(shape) - 2)


def pack_gy_kernel(*refs):
    given, kept = refs[:11], refs[11:20]
    g_ref, side_ref, corner_ref, line_ref, sems = refs[20:]
    copies = [
        pltpu.make_async_copy(source, target, sems.at[n])
        for n, (source, target) in enumerate(zip(given, (*kept, side_ref, corner_ref)))
    ]
    for copy in copies:
        copy.start()
    for copy in copies:
        copy.wait()
    line_ref[0:2, 0:48] = side_ref[0].astype(F32)
    line_ref[2:6, 0:8] = corner_ref[0].astype(F32)
    small = line_ref[0:1, :]
    lane1 = lanes_of((1, 128))
    for row, start in ((1, 48), (2, 96), (4, 104), (3, 112), (5, 120)):
        small = jnp.where(lane1 < start, small, pltpu.roll(line_ref[row : row + 1, :], start, 1))
    g_ref[G_LIST:G_ROWS, :] = jnp.broadcast_to(small, (8, 128))
    lane = lanes_of((8, 128))
    first = lane < 32
    low_level = lane % 32 < 16
    for f in range(FIELDS):
        ref = kept[2 + f]
        parts = [ref[k * 16 : k * 16 + 16, :] for k in range(SD - 1, -1, -1)]
        block = jnp.concatenate(parts, 0)
        if f == 5:
            block = block.astype(F32)
        turned = jnp.transpose(block)
        out = []
        for base, row in ((0, 127), (32, 0)):
            line = jnp.broadcast_to(turned[row : row + 1, :], (8, 128))
            line = pltpu.roll(line, 16, 1, stride=16, stride_axis=0)
            lev0 = pltpu.roll(line, base + 4, 1)
            lev1 = pltpu.roll(line, base + 12, 1)
            out.append(jnp.where(low_level, lev0, lev1))
        block = jnp.where(first, out[0], out[1])
        if f < 4:
            air = kept[f // 2][8 * (f % 2) : 8 * (f % 2) + 8, :]
            block = jnp.where(lane < 64, block, pltpu.roll(air, 67, 1))
        g_ref[f * 8 : f * 8 + 8, :] = block


def pack_gx_kernel(
    q_ref, t_ref, sz_ref, wt_ref, dn_ref, ox_ref, oy_ref, pm_ref, list_ref, near_ref, far_ref,
    east_ref, west_ref, rim_ref,
):
    even = lax.axis_index("gy") % 2 == 0
    lane = lanes_of((8, 128))
    slot = lane % 16
    from_near = (((lane >= 32) & (lane < 64)) | (lane >= 67)) == even
    blocks = []
    for f in range(FIELDS):
        rows = slice(8 * f, 8 * f + 8)
        near = jnp.where(even, near_ref[1, rows, :], near_ref[0, rows, :])
        merged = jnp.where(from_near, near, far_ref[rows, :])
        rim_ref[rows, :] = merged
        blocks.append(merged)
    from_near = (((lane >= 48) & (lane < 96)) | (lane >= 112)) == even
    near = jnp.where(even, near_ref[1, G_LIST:G_ROWS, :], near_ref[0, G_LIST:G_ROWS, :])
    small = jnp.where(from_near, near, far_ref[G_LIST:G_ROWS, :])
    rim_ref[G_LIST:G_ROWS, :] = small
    drops = (sz_ref, wt_ref, dn_ref, ox_ref, oy_ref, pm_ref)
    for side, (out_ref, i, row) in enumerate(((east_ref, 7, 5), (west_ref, 0, 0))):
        for f, ref in enumerate(drops):
            face = ref[pl.ds(i, 16, stride=8), :]
            if f == 5:
                face = face.astype(F32)
            out_ref[16 * f : 16 * f + 16, :] = face
        for g in range(4):
            ref = (q_ref, t_ref)[g // 2]
            at = 8 * (g % 2) + row
            out_ref[X_AIR + 3 * g : X_AIR + 3 * g + 3, :] = ref[at : at + 3, :]
        out_ref[X_AIR + 12 : X_AIR + 16, :] = jnp.zeros((4, 128), F32)
        corner = small
        for g in range(4):
            here = (lane >= 64 + 8 * g) & (lane < 72 + 8 * g)
            corner = jnp.where(here, shift(blocks[g], 8 * g, 1), corner)
        for f in range(FIELDS):
            here = (lane < 64) & (slot == f)
            corner = jnp.where(here, shift(blocks[f], f - 4 - i, 1), corner)
        out_ref[X_CORNER : X_CORNER + 8, :] = corner
        for c in range(8):
            piece = list_ref[0, side : side + 1, 128 * c : 128 * c + 128]
            out_ref[X_LIST + c : X_LIST + c + 1, :] = piece.astype(F32)


def one_hot(values, rows):
    shape = (rows, values.shape[1])
    hit = jnp.broadcast_to(values, shape) == rows_of(shape)
    return jnp.where(hit, 1.0, 0.0).astype(jnp.bfloat16)


def counts(rows, columns):
    return lax.dot_general(rows, columns, (((1,), (1,)), ((), ())), preferred_element_type=F32)


def departed_kernel(list_ref, g_ref, mask_ref):
    entry = g_ref[G_LIST : G_LIST + 1, :].astype(I32)
    mask_ref[...] = counts(one_hot(entry >> 7, 128), one_hot(entry & 127, 128))
    for side, i in ((0, 7), (1, 0)):
        entry = list_ref[0, side : side + 1, :]
        found = counts(one_hot(entry >> 10, 16), one_hot(entry & 127, 128))
        rows = pl.ds(i, 16, stride=8)
        mask_ref[rows, :] = mask_ref[rows, :] + found


def grow(size, dry, forcing):
    initial = size * size
    lowest = dry * dry
    solute = KAPPA_SOLUTE * lowest * dry
    target = initial + GROWTH_STEP * forcing
    upper = (2.5 * GROWTH_STEP) * solute
    lower = (1.5 * GROWTH_STEP) * solute
    wetted = initial
    for _ in range(NEWTON):
        power = wetted * wetted * (wetted * lax.rsqrt(wetted))
        wetted = jnp.maximum((target * power + upper * wetted) / (power + lower), lowest)
    return wetted


def pick(values, bits):
    low, mid, high = bits
    a = [jnp.where(low, values[2 * n + 1], values[2 * n]) for n in range(4)]
    b = [jnp.where(mid, a[2 * n + 1], a[2 * n]) for n in range(2)]
    return jnp.where(high, b[1], b[0])


def coalesce(grown, mult, order):
    bits = [((o & 1) == 1, (o & 2) == 2, o >= 4) for o in order]
    changed = []
    for pair in range(SD // 2):
        first, second = order[2 * pair], order[2 * pair + 1]
        p, q = bits[2 * pair], bits[2 * pair + 1]
        r1, r2 = pick(grown, p), pick(grown, q)
        m1, m2 = pick(mult, p), pick(mult, q)
        big = m1 >= m2
        hr, lr = jnp.where(big, r1, r2), jnp.where(big, r2, r1)
        hm, lm = jnp.where(big, m1, m2), jnp.where(big, m2, m1)
        total = r1 + r2
        rate = COLLIDE_RATE * hm * (total * total) * jnp.abs(r1 * r1 - r2 * r2)
        chance = 1.0 - jnp.exp(-rate)
        volume = lr * lr * lr + chance * (hr * hr * hr)
        merged = jnp.exp2(jnp.log2(volume) * (1.0 / 3.0))
        reduced = hm - chance * lm
        high, low = jnp.where(big, first, second), jnp.where(big, second, first)
        changed.append((high, low, merged, reduced))
    out_radius, out_mult = [], []
    for target in range(SD):
        r, m = grown[target], mult[target]
        for high, low, merged, reduced in changed:
            r = jnp.where(low == target, merged, r)
            m = jnp.where(high == target, reduced, m)
        out_radius.append(r)
        out_mult.append(m)
    return out_radius, out_mult


def droplets(windows, size, mult, dry, east, north, order):
    lines = [(w[1], w[0] - w[1], w[2] - w[1]) for w in windows]
    middle = lines[1]
    below = [x - y for x, y in zip(lines[0], middle)]
    above = [x - y for x, y in zip(lines[2], middle)]
    total = [[None] * 3 for _ in range(3)]
    grown = []
    for k in range(SD):
        dx, dy = east[k] - 0.5, north[k] - 0.5
        ahead_x, ahead_y = dx > 0.0, dy > 0.0
        along, across = jnp.abs(dx), jnp.abs(dy)
        outer = [jnp.where(ahead_x, x, y) for x, y in zip(above, below)]
        forcing = middle[0] + across * jnp.where(ahead_y, middle[2], middle[1])
        forcing = forcing + along * (outer[0] + across * jnp.where(ahead_y, outer[2], outer[1]))
        forcing = forcing - CURVATURE / size[k]
        wetted = grow(size[k], dry[k], forcing)
        radius = wetted * lax.rsqrt(wetted)
        condensed = mult[k] * (wetted * radius - size[k] * size[k] * size[k])
        up_x, up_y = jnp.maximum(dx, 0.0), jnp.maximum(dy, 0.0)
        down_x, down_y = up_x - dx, up_y - dy
        row = (condensed, condensed * down_y, condensed * up_y)
        for a, factor in enumerate((None, down_x, up_x)):
            for b in range(3):
                term = row[b] if factor is None else row[b] * factor
                total[a][b] = term if k == 0 else total[a][b] + term
        grown.append(radius)
    total = [(t[1], t[0] - t[1] - t[2], t[2]) for t in total]
    deposit = [
        total[1],
        tuple(x - y - z for x, y, z in zip(*total)),
        total[2],
    ]
    radius, coalesced = coalesce(grown, mult, order)
    return radius, coalesced, deposit


def physics_kernel(
    q_ref, t_ref, sz_ref, wt_ref, dn_ref, ox_ref, oy_ref, pm_ref, mask_ref,
    rim_ref, west_ref, east_ref,
    moist_out, warm_out, size_out, mult_out, record_out, box_out,
    moist_ref, warm_ref, size_ref, mult_ref, record_ref, box_ref,
    halo_ref, table_ref, air_ref, sems,
):
    leaving = [
        pltpu.make_async_copy(source, target, sems.at[n])
        for n, (source, target) in enumerate((
            (moist_ref, moist_out), (warm_ref, warm_out), (size_ref, size_out),
            (mult_ref, mult_out), (record_ref, record_out), (box_ref, box_out),
        ))
    ]
    lane = lanes_of((8, 128))
    row8 = rows_of((8, 128))
    slot = lane % 16

    air = []
    for a, own_ref in enumerate((q_ref, t_ref)):
        levels = []
        for l in range(2):
            g = 2 * a + l
            row = X_AIR + 3 * g
            air_ref[g, 4:12, :128] = own_ref[8 * l : 8 * l + 8, :]
            air_ref[g, 4:12, 128:] = shift(rim_ref[8 * g : 8 * g + 8, :], -67, 1)
            air_ref[g, 1:4, :128] = west_ref[row : row + 3, :]
            air_ref[g, 1:4, 128:] = shift(west_ref[X_CORNER : X_CORNER + 8, :], -67 - 8 * g, 1)[5:8, :]
            air_ref[g, 12:15, :128] = east_ref[row : row + 3, :]
            air_ref[g, 12:15, 128:] = shift(east_ref[X_CORNER : X_CORNER + 8, :], -67 - 8 * g, 1)[0:3, :]
            levels.append(air_ref[g])
        air.append(levels)
    mixed = []
    for a in range(2):
        both = []
        for l in range(2):
            x = air[a][l]
            other = air[a][1 - l]
            across = (
                shift(x, 1, 0) + shift(x, -1, 0) + shift(x, 1, 1) + shift(x, -1, 1) - 4.0 * x
            )
            both.append(x + MIX_HORIZONTAL * across + MIX_VERTICAL * (other + x - 2.0 * x))
        mixed.append(both)
    moved = []
    turned = []
    for l in range(2):
        vapour, warm = mixed[0][l], mixed[1][l]
        most = EXCESS_FACTOR * jnp.exp(17.27 * (warm - 273.15) / (warm - 35.86))
        humid = vapour / most - 1.0
        columns = [shift(humid, 1, 1), humid, shift(humid, -1, 1)]
        moved.append([[shift(c[:, :128], 1, 0) for c in columns],
                      [c[:, :128] for c in columns],
                      [shift(c[:, :128], -1, 0) for c in columns]])
        ahead = shift(humid, 2, 1)
        tall = lanes_of((16, 128))
        turned.append(jnp.where(tall < 8, ahead[:, :128], shift(ahead[:, 128:], 8, 1)))
    strip = jnp.concatenate(turned + turned + turned + turned, 0)
    strip = jnp.transpose(strip)
    lane1 = lanes_of((1, 128))
    rim = []
    for b in range(3):
        line = jnp.where(lane1 < 32, strip[b : b + 1, :], strip[b + 9 : b + 10, :])
        rim.append([shift(line, 1, 1), line, shift(line, -1, 1)])

    beyond = []
    for f in range(FIELDS):
        line = jnp.where(
            slot == 3,
            shift(west_ref[X_CORNER : X_CORNER + 8, :], 3 - f, 1),
            jnp.where(
                slot == 12,
                shift(east_ref[X_CORNER : X_CORNER + 8, :], 12 - f, 1),
                rim_ref[8 * f : 8 * f + 8, :],
            ),
        )
        line = jnp.where((lane < 64) & (slot >= 3) & (slot <= 12), line, 0.0 if f == 5 else 0.5)
        beyond.append(line)
        for l in range(2):
            base = 16 * f + l
            halo_ref[f, pl.ds(l, 8, stride=8), :] = west_ref[pl.ds(base, 8, stride=2), :]
            halo_ref[f, pl.ds(2 + l, 8, stride=8), :] = east_ref[pl.ds(base, 8, stride=2), :]
        for r in range(4, 8):
            halo_ref[f, pl.ds(r, 8, stride=8), :] = line

    windows = []
    for a in range(3):
        line = []
        for b in range(3):
            line.append(jnp.concatenate(
                [moved[0][a][b][3:4, :], moved[1][a][b][3:4, :],
                 moved[0][a][b][12:13, :], moved[1][a][b][12:13, :]] + [rim[b][a]] * 4, 0))
        windows.append(line)
    tiles = [[halo_ref[f, 8 * k : 8 * k + 8, :] for k in range(SD)] for f in range(5)]
    order = [halo_ref[5, 8 * k : 8 * k + 8, :].astype(I32) for k in range(SD)]
    halo_radius, halo_mult, outer = droplets(windows, *tiles, order)
    for k in range(SD):
        table_ref[0, 8 * k : 8 * k + 8, :] = halo_radius[k]
        table_ref[1, 8 * k : 8 * k + 8, :] = halo_mult[k]

    for side, (ref, dx) in enumerate(((west_ref, 1), (east_ref, -1))):
        entry = ref[X_LIST : X_LIST + 8, :].astype(I32)
        live = entry >= 0
        column = entry & 127
        group = entry >> 10
        picked = [jnp.zeros((8, 128), F32) for _ in range(5)]
        for k in range(SD):
            for l in range(2):
                here = live & (group == 2 * k + l)
                r = 8 * k + 2 * side + l
                for n in range(5):
                    src = table_ref if n < 2 else halo_ref
                    line = jnp.broadcast_to(src[n, r : r + 1, :], (8, 128))
                    got = jnp.take_along_axis(line, column, axis=1)
                    picked[n] = jnp.where(here, got, picked[n])
        box = (((entry >> 10) & 1) * 8 + (((entry >> 7) + dx) & 7)) * 128 + column
        box = jnp.where(live, box, -1)
        for c in range(8):
            at = side * 1024 + c * 128
            for n in range(5):
                record_ref[n, 0:1, at : at + 128] = picked[n][c : c + 1, :]
            box_ref[0:1, at : at + 128] = box[c : c + 1, :]

    diagonal = lane >= 96
    by_west = diagonal & (lane % 16 < 8)
    entry = jnp.where(
        by_west,
        west_ref[X_CORNER : X_CORNER + 8, :],
        jnp.where(diagonal, east_ref[X_CORNER : X_CORNER + 8, :], rim_ref[G_LIST:G_ROWS, :]),
    ).astype(I32)
    live = entry >= 0
    north_side = ((lane >= 48) & (lane < 96)) | (lane >= 112)
    column = entry & 127
    i = (entry >> 7) & 7
    level = (entry >> 10) & 1
    place = i + 4 + jnp.where(diagonal, jnp.where(by_west, -8, 8), 0)
    at = (jnp.where(north_side, 32, 0) + level * 16 + place) & 127
    mine = live & ((entry >> 11) == row8)
    dx = jnp.where(diagonal, jnp.where(by_west, 1, -1), 0)
    dy = jnp.where(north_side, -1, 1)
    box = (level * 8 + ((i + dx) & 7)) * 128 + ((column + dy) & 127)
    box_ref[0:1, 2048:2176] = jnp.where(live, box, -1)[0:1, :]
    for n in range(5):
        if n < 2:
            table = table_ref[n, pl.ds(4, 8, stride=8), :]
        else:
            table = beyond[n]
        got = jnp.take_along_axis(table, at, axis=1)
        line = jnp.sum(jnp.where(mine, got, 0.0), axis=0, keepdims=True)
        record_ref[n, 0:1, 2048:2176] = line
    leaving[4].start()
    leaving[5].start()

    deposits = []
    for l in range(2):
        windows = [[moved[l][a][b][4:12, :] for b in range(3)] for a in range(3)]
        tiles = [
            [ref[k * 16 + 8 * l : k * 16 + 8 * l + 8, :] for k in range(SD)]
            for ref in (sz_ref, wt_ref, dn_ref, ox_ref, oy_ref, pm_ref)
        ]
        radius, coalesced, deposit = droplets(windows, *tiles)
        for k in range(SD):
            rows = slice(k * 16 + 8 * l, k * 16 + 8 * l + 8)
            size_ref[rows, :] = radius[k]
            mult_ref[rows, :] = jnp.where(mask_ref[rows, :] > 0.5, 0.0, coalesced[k])
        deposits.append(deposit)
    leaving[2].start()
    leaving[3].start()

    def along_y(d, a):
        return (
            d[a][1]
            + jnp.where(lane == 0, 0.0, shift(d[a][2], 1, 1))
            + jnp.where(lane == 127, 0.0, shift(d[a][0], -1, 1))
        )

    from_west = along_y(outer, 2)
    from_east = along_y(outer, 0)
    rim_line = [jnp.where(lane1 < 32, outer[a][2][4:5, :], outer[a][0][4:5, :]) for a in range(3)]
    rim_line = shift(rim_line[2], 1, 1) + rim_line[1] + shift(rim_line[0], -1, 1)
    rim_line = jnp.broadcast_to(rim_line, (8, 128))
    for l in range(2):
        own = [along_y(deposits[l], a) for a in range(3)]
        west_row = jnp.broadcast_to(from_west[l : l + 1, :], (8, 128))
        east_row = jnp.broadcast_to(from_east[2 + l : 3 + l, :], (8, 128))
        source = (
            own[1]
            + jnp.where(row8 == 0, west_row, shift(own[2], 1, 0))
            + jnp.where(row8 == 7, east_row, shift(own[0], -1, 0))
        )
        for side, j in enumerate((0, 127)):
            wanted = lane == side * 32 + l * 16 + 4 + row8
            column = jnp.sum(jnp.where(wanted, rim_line, 0.0), axis=1, keepdims=True)
            source = source + jnp.where(lane == j, column, 0.0)
        rows = slice(8 * l, 8 * l + 8)
        moist_ref[rows, :] = mixed[0][l][4:12, :128] - VAPOUR_PER_SOURCE * source
        warm_ref[rows, :] = mixed[1][l][4:12, :128] + WARMING_FACTOR * source
    leaving[0].start()
    leaving[1].start()
    for copy in leaving:
        copy.wait()


def call(kernel, outs, args, scratch=(), space=pltpu.VMEM):
    return pl.pallas_call(
        kernel,
        out_shape=outs,
        in_specs=[pl.BlockSpec(memory_space=pltpu.VMEM)] * len(args),
        out_specs=jax.tree.map(lambda _: pl.BlockSpec(memory_space=space), outs),
        scratch_shapes=list(scratch),
        compiler_params=pltpu.CompilerParams(vmem_limit_bytes=8 << 20),
        cost_estimate=pl.CostEstimate(flops=1 << 20, bytes_accessed=1 << 18, transcendentals=0),
    )(*args)


def ring(axis, step):
    count = lax.axis_size(axis)
    return [(i, (i + step) % count) for i in range(count)]


def swaps(axis, first):
    count = lax.axis_size(axis)
    pairs = [(i % count, (i + 1) % count) for i in range(first, count, 2)]
    return pairs + [(target, source) for source, target in pairs]


def per_device(
    moisture_ratio,
    kelvin_warmth,
    droplet_size_micron,
    weighting_factor,
    dry_nucleus_size,
    fractional_offset_east,
    fractional_offset_north,
    encounter_permutation,
    departing_eastwest_lists,
    departing_northsouth_lists,
    departing_diagonal_lists,
):
    def f32(*shape):
        return jax.ShapeDtypeStruct(shape, F32)

    air = (moisture_ratio.reshape(16, 128), kelvin_warmth.reshape(16, 128))
    drops = tuple(
        x.reshape(128, 128)
        for x in (
            droplet_size_micron,
            weighting_factor,
            dry_nucleus_size,
            fractional_offset_east,
            fractional_offset_north,
            encounter_permutation,
        )
    )
    given = (*air, *drops, departing_eastwest_lists)
    short = (departing_northsouth_lists, departing_diagonal_lists)
    *given, east_west, to_gy = pl.pallas_call(
        pack_gy_kernel,
        out_shape=(*(pltpu.VMEM(x.shape, x.dtype) for x in given), pltpu.VMEM((G_ROWS, 128), F32)),
        in_specs=[pl.BlockSpec(memory_space=pltpu.HBM)] * 11,
        out_specs=(pl.BlockSpec(memory_space=pltpu.VMEM),) * 10,
        scratch_shapes=(
            *(pltpu.VMEM(x.shape, x.dtype) for x in short),
            pltpu.VMEM((8, 128), F32),
            pltpu.SemaphoreType.DMA((11,)),
        ),
        compiler_params=pltpu.CompilerParams(vmem_limit_bytes=8 << 20),
        cost_estimate=pl.CostEstimate(flops=1 << 20, bytes_accessed=1 << 18, transcendentals=0),
    )(*(pltpu.with_memory_space_constraint(x, pltpu.HBM) for x in (*given, *short)))
    far = lax.ppermute(to_gy, "gy", swaps("gy", 1))
    count = lax.axis_size("gy")
    near = lax.all_gather(to_gy, "gy", axis_index_groups=[[i, i + 1] for i in range(0, count, 2)])
    departed = call(departed_kernel, f32(128, 128), (east_west, to_gy))
    to_east, to_west, rim = call(
        pack_gx_kernel,
        (f32(X_ROWS, 128), f32(X_ROWS, 128), f32(G_ROWS, 128)),
        (*given, east_west, near, far),
    )
    from_west = lax.ppermute(to_east, "gx", ring("gx", 1))
    from_east = lax.ppermute(to_west, "gx", ring("gx", -1))
    outs = (
        f32(16, 128),
        f32(16, 128),
        f32(128, 128),
        f32(128, 128),
        f32(5, 1, 2176),
        jax.ShapeDtypeStruct((1, 2176), I32),
    )
    moist, warm, size, mult, records, box = call(
        physics_kernel,
        outs,
        (*given, departed, rim, from_west, from_east),
        scratch=(
            *(pltpu.VMEM(x.shape, x.dtype) for x in outs),
            pltpu.VMEM((FIELDS, 64, 128), F32),
            pltpu.VMEM((2, 64, 128), F32),
            pltpu.VMEM((4, 16, 256), F32),
            pltpu.SemaphoreType.DMA((6,)),
        ),
        space=pltpu.HBM,
    )
    return (
        moist.reshape(moisture_ratio.shape),
        warm.reshape(kelvin_warmth.shape),
        size.reshape(droplet_size_micron.shape),
        mult.reshape(weighting_factor.shape),
        records,
        box,
    )


def solution(mesh):
    cells = P(None, "gx", "gy")
    drop = P(None, None, "gx", "gy")
    lists = P("gx", None, "gy")
    return jax.shard_map(
        per_device,
        mesh=mesh,
        in_specs=(cells,) * 2 + (drop,) * 6 + (lists,) * 3,
        out_specs=(cells, cells, drop, drop, P(None, "gx", "gy"), P("gx", "gy")),
        check_vma=False,
    )
```

```python
import jax
import jax.numpy as jnp
from jax import lax
from jax.experimental import pallas as pl
from jax.experimental.pallas import tpu as pltpu
from jax.sharding import PartitionSpec as P


NEWTON = 4
MIX_HORIZONTAL = 0.2
MIX_VERTICAL = 0.05
EXCESS_FACTOR = 4.2222
CURVATURE = 0.0012
KAPPA_SOLUTE = 0.6
GROWTH_STEP = 200.0
COLLIDE_RATE = 4e-07
VAPOUR_PER_SOURCE = 0.001
WARMING_FACTOR = 0.00249

F32 = jnp.float32
I32 = jnp.int32
SD = 8
FIELDS = 6

G_LIST = 8 * FIELDS
G_ROWS = G_LIST + 8
X_AIR = 16 * FIELDS
X_CORNER = X_AIR + 16
X_LIST = X_CORNER + 8
X_ROWS = X_LIST + 8


def lanes_of(shape):
    return lax.broadcasted_iota(I32, shape, len(shape) - 1)


def shift(x, amount, axis):
    return pltpu.roll(x, amount % x.shape[axis], axis)


def rows_of(shape):
    return lax.broadcasted_iota(I32, shape, len(shape) - 2)


def pack_gy_kernel(*refs):
    given, kept = refs[:11], refs[11:20]
    g_ref, side_ref, corner_ref, line_ref, sems = refs[20:]
    copies = [
        pltpu.make_async_copy(source, target, sems.at[n])
        for n, (source, target) in enumerate(zip(given, (*kept, side_ref, corner_ref)))
    ]
    for copy in copies:
        copy.start()
    for copy in copies:
        copy.wait()
    line_ref[0:2, 0:48] = side_ref[0].astype(F32)
    line_ref[2:6, 0:8] = corner_ref[0].astype(F32)
    small = line_ref[0:1, :]
    lane1 = lanes_of((1, 128))
    for row, start in ((1, 48), (2, 96), (4, 104), (3, 112), (5, 120)):
        small = jnp.where(lane1 < start, small, pltpu.roll(line_ref[row : row + 1, :], start, 1))
    g_ref[G_LIST:G_ROWS, :] = jnp.broadcast_to(small, (8, 128))
    lane = lanes_of((8, 128))
    first = lane < 32
    low_level = lane % 32 < 16
    for f in range(FIELDS):
        ref = kept[2 + f]
        parts = [ref[k * 16 : k * 16 + 16, :] for k in range(SD - 1, -1, -1)]
        block = jnp.concatenate(parts, 0)
        if f == 5:
            block = block.astype(F32)
        turned = jnp.transpose(block)
        out = []
        for base, row in ((0, 127), (32, 0)):
            line = jnp.broadcast_to(turned[row : row + 1, :], (8, 128))
            line = pltpu.roll(line, 16, 1, stride=16, stride_axis=0)
            lev0 = pltpu.roll(line, base + 4, 1)
            lev1 = pltpu.roll(line, base + 12, 1)
            out.append(jnp.where(low_level, lev0, lev1))
        block = jnp.where(first, out[0], out[1])
        if f < 4:
            air = kept[f // 2][8 * (f % 2) : 8 * (f % 2) + 8, :]
            block = jnp.where(lane < 64, block, pltpu.roll(air, 67, 1))
        g_ref[f * 8 : f * 8 + 8, :] = block


def pack_gx_kernel(
    q_ref, t_ref, sz_ref, wt_ref, dn_ref, ox_ref, oy_ref, pm_ref, list_ref, near_ref, far_ref,
    east_ref, west_ref, rim_ref,
):
    even = lax.axis_index("gy") % 2 == 0
    lane = lanes_of((8, 128))
    slot = lane % 16
    from_near = (((lane >= 32) & (lane < 64)) | (lane >= 67)) == even
    blocks = []
    for f in range(FIELDS):
        rows = slice(8 * f, 8 * f + 8)
        near = jnp.where(even, near_ref[1, rows, :], near_ref[0, rows, :])
        merged = jnp.where(from_near, near, far_ref[rows, :])
        rim_ref[rows, :] = merged
        blocks.append(merged)
    from_near = (((lane >= 48) & (lane < 96)) | (lane >= 112)) == even
    near = jnp.where(even, near_ref[1, G_LIST:G_ROWS, :], near_ref[0, G_LIST:G_ROWS, :])
    small = jnp.where(from_near, near, far_ref[G_LIST:G_ROWS, :])
    rim_ref[G_LIST:G_ROWS, :] = small
    drops = (sz_ref, wt_ref, dn_ref, ox_ref, oy_ref, pm_ref)
    for side, (out_ref, i, row) in enumerate(((east_ref, 7, 5), (west_ref, 0, 0))):
        for f, ref in enumerate(drops):
            face = ref[pl.ds(i, 16, stride=8), :]
            if f == 5:
                face = face.astype(F32)
            out_ref[16 * f : 16 * f + 16, :] = face
        for g in range(4):
            ref = (q_ref, t_ref)[g // 2]
            at = 8 * (g % 2) + row
            out_ref[X_AIR + 3 * g : X_AIR + 3 * g + 3, :] = ref[at : at + 3, :]
        out_ref[X_AIR + 12 : X_AIR + 16, :] = jnp.zeros((4, 128), F32)
        corner = small
        for g in range(4):
            here = (lane >= 64 + 8 * g) & (lane < 72 + 8 * g)
            corner = jnp.where(here, shift(blocks[g], 8 * g, 1), corner)
        for f in range(FIELDS):
            here = (lane < 64) & (slot == f)
            corner = jnp.where(here, shift(blocks[f], f - 4 - i, 1), corner)
        out_ref[X_CORNER : X_CORNER + 8, :] = corner
        for c in range(8):
            piece = list_ref[0, side : side + 1, 128 * c : 128 * c + 128]
            out_ref[X_LIST + c : X_LIST + c + 1, :] = piece.astype(F32)


def one_hot(values, rows):
    shape = (rows, values.shape[1])
    hit = jnp.broadcast_to(values, shape) == rows_of(shape)
    return jnp.where(hit, 1.0, 0.0).astype(jnp.bfloat16)


def counts(rows, columns):
    return lax.dot_general(rows, columns, (((1,), (1,)), ((), ())), preferred_element_type=F32)


def departed_kernel(list_ref, g_ref, mask_ref):
    entry = g_ref[G_LIST : G_LIST + 1, :].astype(I32)
    mask_ref[...] = counts(one_hot(entry >> 7, 128), one_hot(entry & 127, 128))
    for side, i in ((0, 7), (1, 0)):
        entry = list_ref[0, side : side + 1, :]
        found = counts(one_hot(entry >> 10, 16), one_hot(entry & 127, 128))
        rows = pl.ds(i, 16, stride=8)
        mask_ref[rows, :] = mask_ref[rows, :] + found


def grow(size, dry, forcing):
    initial = size * size
    lowest = dry * dry
    solute = KAPPA_SOLUTE * lowest * dry
    target = initial + GROWTH_STEP * forcing
    upper = (2.5 * GROWTH_STEP) * solute
    lower = (1.5 * GROWTH_STEP) * solute
    wetted = initial
    for _ in range(NEWTON):
        power = wetted * wetted * (wetted * lax.rsqrt(wetted))
        wetted = jnp.maximum((target * power + upper * wetted) / (power + lower), lowest)
    return wetted


def pick(values, bits):
    low, mid, high = bits
    a = [jnp.where(low, values[2 * n + 1], values[2 * n]) for n in range(4)]
    b = [jnp.where(mid, a[2 * n + 1], a[2 * n]) for n in range(2)]
    return jnp.where(high, b[1], b[0])


def coalesce(grown, mult, order):
    bits = [((o & 1) == 1, (o & 2) == 2, o >= 4) for o in order]
    changed = []
    for pair in range(SD // 2):
        first, second = order[2 * pair], order[2 * pair + 1]
        p, q = bits[2 * pair], bits[2 * pair + 1]
        r1, r2 = pick(grown, p), pick(grown, q)
        m1, m2 = pick(mult, p), pick(mult, q)
        big = m1 >= m2
        hr, lr = jnp.where(big, r1, r2), jnp.where(big, r2, r1)
        hm, lm = jnp.where(big, m1, m2), jnp.where(big, m2, m1)
        total = r1 + r2
        rate = COLLIDE_RATE * hm * (total * total) * jnp.abs(r1 * r1 - r2 * r2)
        chance = 1.0 - jnp.exp(-rate)
        volume = lr * lr * lr + chance * (hr * hr * hr)
        merged = jnp.exp2(jnp.log2(volume) * (1.0 / 3.0))
        reduced = hm - chance * lm
        high, low = jnp.where(big, first, second), jnp.where(big, second, first)
        changed.append((high, low, merged, reduced))
    out_radius, out_mult = [], []
    for target in range(SD):
        r, m = grown[target], mult[target]
        for high, low, merged, reduced in changed:
            r = jnp.where(low == target, merged, r)
            m = jnp.where(high == target, reduced, m)
        out_radius.append(r)
        out_mult.append(m)
    return out_radius, out_mult


def droplets(windows, size, mult, dry, east, north, order):
    lines = [(w[1], w[0] - w[1], w[2] - w[1]) for w in windows]
    middle = lines[1]
    below = [x - y for x, y in zip(lines[0], middle)]
    above = [x - y for x, y in zip(lines[2], middle)]
    total = [[None] * 3 for _ in range(3)]
    grown = []
    for k in range(SD):
        dx, dy = east[k] - 0.5, north[k] - 0.5
        ahead_x, ahead_y = dx > 0.0, dy > 0.0
        along, across = jnp.abs(dx), jnp.abs(dy)
        outer = [jnp.where(ahead_x, x, y) for x, y in zip(above, below)]
        forcing = middle[0] + across * jnp.where(ahead_y, middle[2], middle[1])
        forcing = forcing + along * (outer[0] + across * jnp.where(ahead_y, outer[2], outer[1]))
        forcing = forcing - CURVATURE / size[k]
        wetted = grow(size[k], dry[k], forcing)
        radius = wetted * lax.rsqrt(wetted)
        condensed = mult[k] * (wetted * radius - size[k] * size[k] * size[k])
        up_x, up_y = jnp.maximum(dx, 0.0), jnp.maximum(dy, 0.0)
        down_x, down_y = up_x - dx, up_y - dy
        row = (condensed, condensed * down_y, condensed * up_y)
        for a, factor in enumerate((None, down_x, up_x)):
            for b in range(3):
                term = row[b] if factor is None else row[b] * factor
                total[a][b] = term if k == 0 else total[a][b] + term
        grown.append(radius)
    total = [(t[1], t[0] - t[1] - t[2], t[2]) for t in total]
    deposit = [
        total[1],
        tuple(x - y - z for x, y, z in zip(*total)),
        total[2],
    ]
    radius, coalesced = coalesce(grown, mult, order)
    return radius, coalesced, deposit


def mix(x, other):
    across = shift(x, 1, 0) + shift(x, -1, 0) + shift(x, 1, 1) + shift(x, -1, 1) - 4.0 * x
    return x + MIX_HORIZONTAL * across + MIX_VERTICAL * (other + x - 2.0 * x)


def moisture_excess(vapour, warm):
    most = EXCESS_FACTOR * jnp.exp(17.27 * (warm - 273.15) / (warm - 35.86))
    return vapour / most - 1.0


def stencil(humid):
    columns = [shift(humid, 1, 1)[:, :128], humid[:, :128], shift(humid, -1, 1)[:, :128]]
    return [[shift(c, 1, 0) for c in columns], columns, [shift(c, -1, 0) for c in columns]]


def along_y(d, a):
    lane = lanes_of((8, 128))
    return (
        d[a][1]
        + jnp.where(lane == 0, 0.0, shift(d[a][2], 1, 1))
        + jnp.where(lane == 127, 0.0, shift(d[a][0], -1, 1))
    )


def face_records(list_rows, step, first_row, table_ref, halo_ref, record_ref, box_ref):
    entry = list_rows.astype(I32)
    live = entry >= 0
    column = entry & 127
    group = entry >> 10
    picked = [jnp.zeros((8, 128), F32) for _ in range(5)]
    for k in range(SD):
        for l in range(2):
            here = live & (group == 2 * k + l)
            r = 8 * k + first_row + l
            for n in range(5):
                src = table_ref if n < 2 else halo_ref
                line = jnp.broadcast_to(src[n, r : r + 1, :], (8, 128))
                got = jnp.take_along_axis(line, column, axis=1)
                picked[n] = jnp.where(here, got, picked[n])
    box = (((entry >> 10) & 1) * 8 + (((entry >> 7) + step) & 7)) * 128 + column
    box = jnp.where(live, box, -1)
    for c in range(8):
        lanes = slice(c * 128, c * 128 + 128)
        for n in range(5):
            record_ref[n, 0:1, lanes] = picked[n][c : c + 1, :]
        box_ref[0:1, lanes] = box[c : c + 1, :]


def west_kernel(
    q_ref, t_ref, sz_ref, wt_ref, dn_ref, ox_ref, oy_ref, pm_ref, mask_ref, rim_ref, west_ref,
    size_ref, mult_ref, humid_ref, mixed_ref, source_ref, record_ref, box_ref,
    halo_ref, table_ref, air_ref,
):
    row8 = rows_of((8, 128))
    for a, own_ref in enumerate((q_ref, t_ref)):
        for l in range(2):
            g = 2 * a + l
            row = X_AIR + 3 * g
            side = shift(west_ref[X_CORNER : X_CORNER + 8, :], -67 - 8 * g, 1)
            air_ref[g, 4:12, :128] = own_ref[8 * l : 8 * l + 8, :]
            air_ref[g, 4:12, 128:] = shift(rim_ref[8 * g : 8 * g + 8, :], -67, 1)
            air_ref[g, 1:4, :128] = west_ref[row : row + 3, :]
            air_ref[g, 1:4, 128:] = side[5:8, :]
    moved = []
    for l in range(2):
        vapour = mix(air_ref[l], air_ref[1 - l])
        warm = mix(air_ref[2 + l], air_ref[3 - l])
        mixed_ref[8 * l : 8 * l + 8, :] = vapour[4:12, :128]
        mixed_ref[16 + 8 * l : 24 + 8 * l, :] = warm[4:12, :128]
        humid = moisture_excess(vapour, warm)
        humid_ref[8 * l : 8 * l + 8, :] = humid[0:8, :]
        moved.append(stencil(humid))

    for f in range(FIELDS):
        for r in range(8):
            halo_ref[f, pl.ds(r, 8, stride=8), :] = west_ref[pl.ds(16 * f + r % 2, 8, stride=2), :]
    windows = [
        [
            jnp.concatenate([moved[0][a][b][3:4, :], moved[1][a][b][3:4, :]] * 4, 0)
            for b in range(3)
        ]
        for a in range(3)
    ]
    tiles = [[halo_ref[f, 8 * k : 8 * k + 8, :] for k in range(SD)] for f in range(5)]
    order = [halo_ref[5, 8 * k : 8 * k + 8, :].astype(I32) for k in range(SD)]
    halo_radius, halo_mult, outer = droplets(windows, *tiles, order)
    for k in range(SD):
        table_ref[0, 8 * k : 8 * k + 8, :] = halo_radius[k]
        table_ref[1, 8 * k : 8 * k + 8, :] = halo_mult[k]
    face_records(
        west_ref[X_LIST : X_LIST + 8, :], 1, 0, table_ref, halo_ref, record_ref, box_ref
    )

    from_west = along_y(outer, 2)
    for l in range(2):
        windows = [[moved[l][a][b][4:12, :] for b in range(3)] for a in range(3)]
        tiles = [
            [ref[k * 16 + 8 * l : k * 16 + 8 * l + 8, :] for k in range(SD)]
            for ref in (sz_ref, wt_ref, dn_ref, ox_ref, oy_ref, pm_ref)
        ]
        radius, coalesced, deposit = droplets(windows, *tiles)
        for k in range(SD):
            rows = slice(k * 16 + 8 * l, k * 16 + 8 * l + 8)
            size_ref[rows, :] = radius[k]
            mult_ref[rows, :] = jnp.where(mask_ref[rows, :] > 0.5, 0.0, coalesced[k])
        own = [jnp.where(row8 < 6, along_y(deposit, a), 0.0) for a in range(3)]
        west_row = jnp.broadcast_to(from_west[l : l + 1, :], (8, 128))
        source_ref[8 * l : 8 * l + 8, :] = (
            own[1]
            + jnp.where(row8 == 0, west_row, shift(own[2], 1, 0))
            + jnp.where(row8 == 7, 0.0, shift(own[0], -1, 0))
        )


def east_kernel(
    q_ref, t_ref, sz_ref, wt_ref, dn_ref, ox_ref, oy_ref, pm_ref, mask_ref, rim_ref, west_ref,
    east_ref, early_size, early_mult, humid_ref, mixed_ref, source_ref, west_record, west_box,
    moist_out, warm_out, size_out, mult_out, record_out, box_out,
    moist_ref, warm_ref, size_ref, mult_ref, record_ref, box_ref,
    halo_ref, table_ref, air_ref, sems,
):
    leaving = [
        pltpu.make_async_copy(source, target, sems.at[n])
        for n, (source, target) in enumerate((
            (west_record, record_out.at[:, :, 0:1024]), (west_box, box_out.at[:, 0:1024]),
            (size_ref, size_out), (mult_ref, mult_out),
            (record_ref, record_out.at[:, :, 1024:2176]), (box_ref, box_out.at[:, 1024:2176]),
            (moist_ref, moist_out), (warm_ref, warm_out),
        ))
    ]
    leaving[0].start()
    leaving[1].start()
    lane = lanes_of((8, 128))
    lane1 = lanes_of((1, 128))
    row8 = rows_of((8, 128))
    slot = lane % 16
    for a, own_ref in enumerate((q_ref, t_ref)):
        for l in range(2):
            g = 2 * a + l
            row = X_AIR + 3 * g
            side = shift(east_ref[X_CORNER : X_CORNER + 8, :], -67 - 8 * g, 1)
            air_ref[g, 0:5, :128] = own_ref[8 * l + 3 : 8 * l + 8, :]
            air_ref[g, 0:5, 128:] = shift(rim_ref[8 * g : 8 * g + 8, :], -67, 1)[3:8, :]
            air_ref[g, 5:8, :128] = east_ref[row : row + 3, :]
            air_ref[g, 5:8, 128:] = side[0:3, :]
    mixed = []
    moved = []
    turned = []
    for l in range(2):
        vapour = mix(air_ref[l], air_ref[1 - l])
        warm = mix(air_ref[2 + l], air_ref[3 - l])
        mixed.append((shift(vapour[:, :128], 3, 0), shift(warm[:, :128], 3, 0)))
        humid = moisture_excess(vapour, warm)
        moved.append(stencil(humid))
        whole = jnp.concatenate([humid_ref[8 * l : 8 * l + 8, :], shift(humid, -1, 0)], 0)
        ahead = shift(whole, 2, 1)
        tall = lanes_of((16, 128))
        turned.append(jnp.where(tall < 8, ahead[:, :128], shift(ahead[:, 128:], 8, 1)))
    strip = jnp.transpose(jnp.concatenate(turned * 4, 0))
    rim = []
    for b in range(3):
        line = jnp.where(lane1 < 32, strip[b : b + 1, :], strip[b + 9 : b + 10, :])
        rim.append([shift(line, 1, 1), line, shift(line, -1, 1)])

    beyond = []
    for f, own_ref in enumerate((sz_ref, wt_ref, dn_ref, ox_ref, oy_ref, pm_ref)):
        line = jnp.where(
            slot == 3,
            shift(west_ref[X_CORNER : X_CORNER + 8, :], 3 - f, 1),
            jnp.where(
                slot == 12,
                shift(east_ref[X_CORNER : X_CORNER + 8, :], 12 - f, 1),
                rim_ref[8 * f : 8 * f + 8, :],
            ),
        )
        line = jnp.where((lane < 64) & (slot >= 3) & (slot <= 12), line, 0.0 if f == 5 else 0.5)
        beyond.append(line)
        for l in range(2):
            for n, i in enumerate((6, 7)):
                own = own_ref[pl.ds(8 * l + i, 8, stride=16), :]
                halo_ref[f, pl.ds(2 * n + l, 8, stride=8), :] = own.astype(F32)
            east = east_ref[pl.ds(16 * f + l, 8, stride=2), :]
            halo_ref[f, pl.ds(4 + l, 8, stride=8), :] = east
            halo_ref[f, pl.ds(6 + l, 8, stride=8), :] = line
    windows = [
        [
            jnp.concatenate(
                [moved[l][a][b][r : r + 1, :] for r in (3, 4, 5) for l in range(2)]
                + [rim[b][a]] * 2,
                0,
            )
            for b in range(3)
        ]
        for a in range(3)
    ]
    tiles = [[halo_ref[f, 8 * k : 8 * k + 8, :] for k in range(SD)] for f in range(5)]
    order = [halo_ref[5, 8 * k : 8 * k + 8, :].astype(I32) for k in range(SD)]
    radius, coalesced, outer = droplets(windows, *tiles, order)
    for k in range(SD):
        table_ref[0, 8 * k : 8 * k + 8, :] = radius[k]
        table_ref[1, 8 * k : 8 * k + 8, :] = coalesced[k]

    size_ref[...] = early_size[...]
    mult_ref[...] = early_mult[...]
    for l in range(2):
        for n, i in enumerate((6, 7)):
            rows = pl.ds(8 * l + i, 8, stride=16)
            at = pl.ds(2 * n + l, 8, stride=8)
            size_ref[rows, :] = table_ref[0, at, :]
            mult_ref[rows, :] = jnp.where(mask_ref[rows, :] > 0.5, 0.0, table_ref[1, at, :])
    leaving[2].start()
    leaving[3].start()

    face_records(
        east_ref[X_LIST : X_LIST + 8, :], -1, 4, table_ref, halo_ref, record_ref, box_ref
    )
    diagonal = lane >= 96
    by_west = diagonal & (lane % 16 < 8)
    entry = jnp.where(
        by_west,
        west_ref[X_CORNER : X_CORNER + 8, :],
        jnp.where(diagonal, east_ref[X_CORNER : X_CORNER + 8, :], rim_ref[G_LIST:G_ROWS, :]),
    ).astype(I32)
    live = entry >= 0
    north_side = ((lane >= 48) & (lane < 96)) | (lane >= 112)
    column = entry & 127
    i = (entry >> 7) & 7
    level = (entry >> 10) & 1
    place = i + 4 + jnp.where(diagonal, jnp.where(by_west, -8, 8), 0)
    at = (jnp.where(north_side, 32, 0) + level * 16 + place) & 127
    mine = live & ((entry >> 11) == row8)
    dx = jnp.where(diagonal, jnp.where(by_west, 1, -1), 0)
    dy = jnp.where(north_side, -1, 1)
    box = (level * 8 + ((i + dx) & 7)) * 128 + ((column + dy) & 127)
    box_ref[0:1, 1024:1152] = jnp.where(live, box, -1)[0:1, :]
    for n in range(5):
        table = table_ref[n, pl.ds(6, 8, stride=8), :] if n < 2 else beyond[n]
        got = jnp.take_along_axis(table, at, axis=1)
        line = jnp.sum(jnp.where(mine, got, 0.0), axis=0, keepdims=True)
        record_ref[n, 0:1, 1024:1152] = line
    leaving[4].start()
    leaving[5].start()

    down, level_row, up = (along_y(outer, a) for a in range(3))
    rim_line = [jnp.where(lane1 < 32, outer[a][2][6:7, :], outer[a][0][6:7, :]) for a in range(3)]
    rim_line = shift(rim_line[2], 1, 1) + rim_line[1] + shift(rim_line[0], -1, 1)
    rim_line = jnp.broadcast_to(rim_line, (8, 128))
    for l in range(2):
        extra = (
            down[l : l + 1, :],
            level_row[l : l + 1, :] + down[2 + l : 3 + l, :],
            up[l : l + 1, :] + level_row[2 + l : 3 + l, :] + down[4 + l : 5 + l, :],
        )
        added = jnp.zeros((8, 128), F32)
        for r, line in zip((5, 6, 7), extra):
            added = jnp.where(row8 == r, jnp.broadcast_to(line, (8, 128)), added)
        rows = slice(8 * l, 8 * l + 8)
        source = source_ref[rows, :] + added
        for side, j in enumerate((0, 127)):
            wanted = lane == side * 32 + l * 16 + 4 + row8
            part = jnp.sum(jnp.where(wanted, rim_line, 0.0), axis=1, keepdims=True)
            source = source + jnp.where(lane == j, part, 0.0)
        vapour = jnp.where(row8 < 4, mixed_ref[rows, :], mixed[l][0])
        warm = jnp.where(row8 < 4, mixed_ref[16 + 8 * l : 24 + 8 * l, :], mixed[l][1])
        moist_ref[rows, :] = vapour - VAPOUR_PER_SOURCE * source
        warm_ref[rows, :] = warm + WARMING_FACTOR * source
    leaving[6].start()
    leaving[7].start()
    for copy in leaving:
        copy.wait()


def call(kernel, outs, args, scratch=(), space=pltpu.VMEM):
    return pl.pallas_call(
        kernel,
        out_shape=outs,
        in_specs=[pl.BlockSpec(memory_space=pltpu.VMEM)] * len(args),
        out_specs=jax.tree.map(lambda _: pl.BlockSpec(memory_space=space), outs),
        scratch_shapes=list(scratch),
        compiler_params=pltpu.CompilerParams(vmem_limit_bytes=8 << 20),
        cost_estimate=pl.CostEstimate(flops=1 << 20, bytes_accessed=1 << 18, transcendentals=0),
    )(*args)


def ring(axis, step):
    count = lax.axis_size(axis)
    return [(i, (i + step) % count) for i in range(count)]


def swaps(axis, first):
    count = lax.axis_size(axis)
    pairs = [(i % count, (i + 1) % count) for i in range(first, count, 2)]
    return pairs + [(target, source) for source, target in pairs]


def per_device(
    moisture_ratio,
    kelvin_warmth,
    droplet_size_micron,
    weighting_factor,
    dry_nucleus_size,
    fractional_offset_east,
    fractional_offset_north,
    encounter_permutation,
    departing_eastwest_lists,
    departing_northsouth_lists,
    departing_diagonal_lists,
):
    def f32(*shape):
        return jax.ShapeDtypeStruct(shape, F32)

    air = (moisture_ratio.reshape(16, 128), kelvin_warmth.reshape(16, 128))
    drops = tuple(
        x.reshape(128, 128)
        for x in (
            droplet_size_micron,
            weighting_factor,
            dry_nucleus_size,
            fractional_offset_east,
            fractional_offset_north,
            encounter_permutation,
        )
    )
    given = (*air, *drops, departing_eastwest_lists)
    short = (departing_northsouth_lists, departing_diagonal_lists)
    *given, east_west, to_gy = pl.pallas_call(
        pack_gy_kernel,
        out_shape=(*(pltpu.VMEM(x.shape, x.dtype) for x in given), pltpu.VMEM((G_ROWS, 128), F32)),
        in_specs=[pl.BlockSpec(memory_space=pltpu.HBM)] * 11,
        out_specs=(pl.BlockSpec(memory_space=pltpu.VMEM),) * 10,
        scratch_shapes=(
            *(pltpu.VMEM(x.shape, x.dtype) for x in short),
            pltpu.VMEM((8, 128), F32),
            pltpu.SemaphoreType.DMA((11,)),
        ),
        compiler_params=pltpu.CompilerParams(vmem_limit_bytes=8 << 20),
        cost_estimate=pl.CostEstimate(flops=1 << 20, bytes_accessed=1 << 18, transcendentals=0),
    )(*(pltpu.with_memory_space_constraint(x, pltpu.HBM) for x in (*given, *short)))
    far = lax.ppermute(to_gy, "gy", swaps("gy", 1))
    count = lax.axis_size("gy")
    near = lax.all_gather(to_gy, "gy", axis_index_groups=[[i, i + 1] for i in range(0, count, 2)])
    departed = call(departed_kernel, f32(128, 128), (east_west, to_gy))
    to_east, to_west, rim = call(
        pack_gx_kernel,
        (f32(X_ROWS, 128), f32(X_ROWS, 128), f32(G_ROWS, 128)),
        (*given, east_west, near, far),
    )
    from_west = lax.ppermute(to_east, "gx", ring("gx", 1))
    from_east = lax.ppermute(to_west, "gx", ring("gx", -1))
    scratch = (pltpu.VMEM((FIELDS, 64, 128), F32), pltpu.VMEM((2, 64, 128), F32))
    early = call(
        west_kernel,
        (
            pltpu.VMEM((128, 128), F32),
            pltpu.VMEM((128, 128), F32),
            pltpu.VMEM((16, 256), F32),
            pltpu.VMEM((32, 128), F32),
            pltpu.VMEM((16, 128), F32),
            pltpu.VMEM((5, 1, 1024), F32),
            pltpu.VMEM((1, 1024), I32),
        ),
        (*given, departed, rim, from_west),
        scratch=(*scratch, pltpu.VMEM((4, 16, 256), F32)),
    )
    moist, warm, size, mult, records, box = call(
        east_kernel,
        (
            f32(16, 128),
            f32(16, 128),
            f32(128, 128),
            f32(128, 128),
            f32(5, 1, 2176),
            jax.ShapeDtypeStruct((1, 2176), I32),
        ),
        (*given, departed, rim, from_west, from_east, *early),
        scratch=(
            pltpu.VMEM((16, 128), F32),
            pltpu.VMEM((16, 128), F32),
            pltpu.VMEM((128, 128), F32),
            pltpu.VMEM((128, 128), F32),
            pltpu.VMEM((5, 1, 1152), F32),
            pltpu.VMEM((1, 1152), I32),
            *scratch,
            pltpu.VMEM((4, 8, 256), F32),
            pltpu.SemaphoreType.DMA((8,)),
        ),
        space=pltpu.HBM,
    )
    return (
        moist.reshape(moisture_ratio.shape),
        warm.reshape(kelvin_warmth.shape),
        size.reshape(droplet_size_micron.shape),
        mult.reshape(weighting_factor.shape),
        records,
        box,
    )


def solution(mesh):
    cells = P(None, "gx", "gy")
    drop = P(None, None, "gx", "gy")
    lists = P("gx", None, "gy")
    return jax.shard_map(
        per_device,
        mesh=mesh,
        in_specs=(cells,) * 2 + (drop,) * 6 + (lists,) * 3,
        out_specs=(cells, cells, drop, drop, P(None, "gx", "gy"), P("gx", "gy")),
        check_vma=False,
    )
```

```python
import jax
import jax.numpy as jnp
from jax import lax
from jax.experimental import pallas as pl
from jax.experimental.pallas import tpu as pltpu
from jax.sharding import PartitionSpec as P


NEWTON = 4
MIX_HORIZONTAL = 0.2
MIX_VERTICAL = 0.05
EXCESS_FACTOR = 4.2222
CURVATURE = 0.0012
KAPPA_SOLUTE = 0.6
GROWTH_STEP = 200.0
COLLIDE_RATE = 4e-07
VAPOUR_PER_SOURCE = 0.001
WARMING_FACTOR = 0.00249

F32 = jnp.float32
I32 = jnp.int32
SD = 8
FIELDS = 6

G_LIST = 8 * FIELDS
G_ROWS = G_LIST + 8
R_EXT = G_ROWS
R_ROWS = R_EXT + 32
X_AIR = 16 * FIELDS
X_EXT = X_AIR + 16
X_CORNER = X_EXT + 16
X_LIST = X_CORNER + 8
X_ROWS = X_LIST + 8


def lanes_of(shape):
    return lax.broadcasted_iota(I32, shape, len(shape) - 1)


def shift(x, amount, axis):
    return pltpu.roll(x, amount % x.shape[axis], axis)


def rows_of(shape):
    return lax.broadcasted_iota(I32, shape, len(shape) - 2)


def pack_gy_kernel(*refs):
    given, kept = refs[:11], refs[11:20]
    g_ref, side_ref, corner_ref, line_ref, sems = refs[20:]
    copies = [
        pltpu.make_async_copy(source, target, sems.at[n])
        for n, (source, target) in enumerate(zip(given, (*kept, side_ref, corner_ref)))
    ]
    for copy in copies:
        copy.start()
    for copy in copies:
        copy.wait()
    line_ref[0:2, 0:48] = side_ref[0].astype(F32)
    line_ref[2:6, 0:8] = corner_ref[0].astype(F32)
    small = line_ref[0:1, :]
    lane1 = lanes_of((1, 128))
    for row, start in ((1, 48), (2, 96), (4, 104), (3, 112), (5, 120)):
        small = jnp.where(lane1 < start, small, pltpu.roll(line_ref[row : row + 1, :], start, 1))
    g_ref[G_LIST:G_ROWS, :] = jnp.broadcast_to(small, (8, 128))
    lane = lanes_of((8, 128))
    first = lane < 32
    low_level = lane % 32 < 16
    for f in range(FIELDS):
        ref = kept[2 + f]
        parts = [ref[k * 16 : k * 16 + 16, :] for k in (0, 7, 6, 5, 4, 3, 2, 1)]
        block = jnp.concatenate(parts, 0)
        if f == 5:
            block = block.astype(F32)
        turned = jnp.transpose(block)
        out = []
        for row in (127, 0):
            line = jnp.broadcast_to(turned[row : row + 1, :], (8, 128))
            lev0 = pltpu.roll(line, 4, 1, stride=16, stride_axis=0)
            lev1 = pltpu.roll(line, 12, 1, stride=16, stride_axis=0)
            out.append(jnp.where(low_level, lev0, lev1))
        out[1] = shift(out[1], -2, 0)
        block = jnp.where(first, out[0], out[1])
        if f < 4:
            air = kept[f // 2][8 * (f % 2) : 8 * (f % 2) + 8, :]
            block = jnp.where(lane < 64, block, pltpu.roll(air, 67, 1))
        g_ref[f * 8 : f * 8 + 8, :] = block


def pack_gx_kernel(
    q_ref, t_ref, sz_ref, wt_ref, dn_ref, ox_ref, oy_ref, pm_ref, list_ref, near_ref, far_ref,
    east_ref, west_ref, rim_ref,
):
    even = lax.axis_index("gy") % 2 == 0
    lane = lanes_of((8, 128))
    slot = lane % 16
    from_near = (((lane >= 32) & (lane < 64)) | (lane >= 67)) == even
    blocks = []
    for f in range(FIELDS):
        rows = slice(8 * f, 8 * f + 8)
        near = jnp.where(even, near_ref[1, rows, :], near_ref[0, rows, :])
        merged = jnp.where(from_near, near, far_ref[rows, :])
        rim_ref[rows, :] = merged
        blocks.append(merged)
    from_near = (((lane >= 48) & (lane < 96)) | (lane >= 112)) == even
    near = jnp.where(even, near_ref[1, G_LIST:G_ROWS, :], near_ref[0, G_LIST:G_ROWS, :])
    small = jnp.where(from_near, near, far_ref[G_LIST:G_ROWS, :])
    rim_ref[G_LIST:G_ROWS, :] = small
    ext = [shift(blocks[g], -67, 1) for g in range(4)]
    for g in range(4):
        rim_ref[R_EXT + 8 * g : R_EXT + 8 * g + 8, :] = ext[g]
    drops = (sz_ref, wt_ref, dn_ref, ox_ref, oy_ref, pm_ref)
    for side, (out_ref, i, row) in enumerate(((east_ref, 7, 5), (west_ref, 0, 0))):
        for f, ref in enumerate(drops):
            face = ref[pl.ds(i, 16, stride=8), :]
            if f == 5:
                face = face.astype(F32)
            out_ref[16 * f : 16 * f + 16, :] = face
        for g in range(4):
            ref = (q_ref, t_ref)[g // 2]
            at = 8 * (g % 2) + row
            out_ref[X_AIR + 3 * g : X_AIR + 3 * g + 3, :] = ref[at : at + 3, :]
            out_ref[X_EXT + 3 * g : X_EXT + 3 * g + 3, :] = ext[g][row : row + 3, :]
        out_ref[X_AIR + 12 : X_AIR + 16, :] = jnp.zeros((4, 128), F32)
        out_ref[X_EXT + 12 : X_EXT + 16, :] = jnp.zeros((4, 128), F32)
        corner = small
        for f in range(FIELDS):
            here = (lane < 64) & (slot == f)
            corner = jnp.where(here, shift(blocks[f], f - 4 - i, 1), corner)
        out_ref[X_CORNER : X_CORNER + 8, :] = corner
        for c in range(8):
            piece = list_ref[0, side : side + 1, 128 * c : 128 * c + 128]
            out_ref[X_LIST + c : X_LIST + c + 1, :] = piece.astype(F32)


def one_hot(values, rows):
    shape = (rows, values.shape[1])
    hit = jnp.broadcast_to(values, shape) == rows_of(shape)
    return jnp.where(hit, 1.0, 0.0).astype(jnp.bfloat16)


def counts(rows, columns):
    return lax.dot_general(rows, columns, (((1,), (1,)), ((), ())), preferred_element_type=F32)


def departed_kernel(list_ref, g_ref, mask_ref):
    entry = g_ref[G_LIST : G_LIST + 1, :].astype(I32)
    mask_ref[...] = counts(one_hot(entry >> 7, 128), one_hot(entry & 127, 128))
    for side, i in ((0, 7), (1, 0)):
        entry = list_ref[0, side : side + 1, :]
        found = counts(one_hot(entry >> 10, 16), one_hot(entry & 127, 128))
        rows = pl.ds(i, 16, stride=8)
        mask_ref[rows, :] = mask_ref[rows, :] + found


def grow(size, dry, forcing):
    initial = size * size
    lowest = dry * dry
    solute = KAPPA_SOLUTE * lowest * dry
    target = initial + GROWTH_STEP * forcing
    upper = (2.5 * GROWTH_STEP) * solute
    lower = (1.5 * GROWTH_STEP) * solute
    wetted = initial
    for _ in range(NEWTON):
        power = wetted * wetted * (wetted * lax.rsqrt(wetted))
        wetted = jnp.maximum((target * power + upper * wetted) / (power + lower), lowest)
    return wetted


def pick(values, bits):
    low, mid, high = bits
    a = [jnp.where(low, values[2 * n + 1], values[2 * n]) for n in range(4)]
    b = [jnp.where(mid, a[2 * n + 1], a[2 * n]) for n in range(2)]
    return jnp.where(high, b[1], b[0])


def coalesce(grown, mult, order):
    bits = [((o & 1) == 1, (o & 2) == 2, o >= 4) for o in order]
    changed = []
    for pair in range(SD // 2):
        first, second = order[2 * pair], order[2 * pair + 1]
        p, q = bits[2 * pair], bits[2 * pair + 1]
        r1, r2 = pick(grown, p), pick(grown, q)
        m1, m2 = pick(mult, p), pick(mult, q)
        big = m1 >= m2
        hr, lr = jnp.where(big, r1, r2), jnp.where(big, r2, r1)
        hm, lm = jnp.where(big, m1, m2), jnp.where(big, m2, m1)
        total = r1 + r2
        rate = COLLIDE_RATE * hm * (total * total) * jnp.abs(r1 * r1 - r2 * r2)
        chance = 1.0 - jnp.exp(-rate)
        volume = lr * lr * lr + chance * (hr * hr * hr)
        merged = jnp.exp2(jnp.log2(volume) * (1.0 / 3.0))
        reduced = hm - chance * lm
        high, low = jnp.where(big, first, second), jnp.where(big, second, first)
        changed.append((high, low, merged, reduced))
    out_radius, out_mult = [], []
    for target in range(SD):
        r, m = grown[target], mult[target]
        for high, low, merged, reduced in changed:
            r = jnp.where(low == target, merged, r)
            m = jnp.where(high == target, reduced, m)
        out_radius.append(r)
        out_mult.append(m)
    return out_radius, out_mult


def droplets(windows, size, mult, dry, east, north, order):
    lines = [(w[1], w[0] - w[1], w[2] - w[1]) for w in windows]
    middle = lines[1]
    below = [x - y for x, y in zip(lines[0], middle)]
    above = [x - y for x, y in zip(lines[2], middle)]
    total = [[None] * 3 for _ in range(3)]
    grown = []
    for k in range(SD):
        dx, dy = east[k] - 0.5, north[k] - 0.5
        ahead_x, ahead_y = dx > 0.0, dy > 0.0
        along, across = jnp.abs(dx), jnp.abs(dy)
        outer = [jnp.where(ahead_x, x, y) for x, y in zip(above, below)]
        forcing = middle[0] + across * jnp.where(ahead_y, middle[2], middle[1])
        forcing = forcing + along * (outer[0] + across * jnp.where(ahead_y, outer[2], outer[1]))
        forcing = forcing - CURVATURE / size[k]
        wetted = grow(size[k], dry[k], forcing)
        radius = wetted * lax.rsqrt(wetted)
        condensed = mult[k] * (wetted * radius - size[k] * size[k] * size[k])
        up_x, up_y = jnp.maximum(dx, 0.0), jnp.maximum(dy, 0.0)
        down_x, down_y = up_x - dx, up_y - dy
        row = (condensed, condensed * down_y, condensed * up_y)
        for a, factor in enumerate((None, down_x, up_x)):
            for b in range(3):
                term = row[b] if factor is None else row[b] * factor
                total[a][b] = term if k == 0 else total[a][b] + term
        grown.append(radius)
    total = [(t[1], t[0] - t[1] - t[2], t[2]) for t in total]
    deposit = [
        total[1],
        tuple(x - y - z for x, y, z in zip(*total)),
        total[2],
    ]
    radius, coalesced = coalesce(grown, mult, order)
    return radius, coalesced, deposit


def mix(x, other):
    across = shift(x, 1, 0) + shift(x, -1, 0) + shift(x, 1, 1) + shift(x, -1, 1) - 4.0 * x
    return x + MIX_HORIZONTAL * across + MIX_VERTICAL * (other + x - 2.0 * x)


def moisture_excess(vapour, warm):
    most = EXCESS_FACTOR * jnp.exp(17.27 * (warm - 273.15) / (warm - 35.86))
    return vapour / most - 1.0


def stencil(humid):
    columns = [shift(humid, 1, 1)[:, :128], humid[:, :128], shift(humid, -1, 1)[:, :128]]
    return [[shift(c, 1, 0) for c in columns], columns, [shift(c, -1, 0) for c in columns]]


def along_y(d, a):
    lane = lanes_of((8, 128))
    return (
        d[a][1]
        + jnp.where(lane == 0, 0.0, shift(d[a][2], 1, 1))
        + jnp.where(lane == 127, 0.0, shift(d[a][0], -1, 1))
    )


def face_records(list_rows, step, first_row, table_ref, halo_ref, record_ref, box_ref):
    entry = list_rows.astype(I32)
    live = entry >= 0
    column = entry & 127
    group = entry >> 10
    picked = [jnp.zeros((8, 128), F32) for _ in range(5)]
    for k in range(SD):
        for l in range(2):
            here = live & (group == 2 * k + l)
            r = 8 * k + first_row + l
            for n in range(5):
                src = table_ref if n < 2 else halo_ref
                line = jnp.broadcast_to(src[n, r : r + 1, :], (8, 128))
                got = jnp.take_along_axis(line, column, axis=1)
                picked[n] = jnp.where(here, got, picked[n])
    box = (((entry >> 10) & 1) * 8 + (((entry >> 7) + step) & 7)) * 128 + column
    box = jnp.where(live, box, -1)
    for c in range(8):
        lanes = slice(c * 128, c * 128 + 128)
        for n in range(5):
            record_ref[n, 0:1, lanes] = picked[n][c : c + 1, :]
        box_ref[0:1, lanes] = box[c : c + 1, :]


def west_kernel(
    q_ref, t_ref, sz_ref, wt_ref, dn_ref, ox_ref, oy_ref, pm_ref, mask_ref, rim_ref, west_ref,
    size_ref, mult_ref, humid_ref, mixed_ref, source_ref, record_ref, box_ref,
    halo_ref, table_ref, air_ref,
):
    row8 = rows_of((8, 128))
    for a, own_ref in enumerate((q_ref, t_ref)):
        for l in range(2):
            g = 2 * a + l
            row = X_AIR + 3 * g
            far = X_EXT + 3 * g
            air_ref[g, 4:12, :128] = own_ref[8 * l : 8 * l + 8, :]
            air_ref[g, 4:12, 128:] = rim_ref[R_EXT + 8 * g : R_EXT + 8 * g + 8, :]
            air_ref[g, 1:4, :128] = west_ref[row : row + 3, :]
            air_ref[g, 1:4, 128:] = west_ref[far : far + 3, :]
    moved = []
    for l in range(2):
        vapour = mix(air_ref[l], air_ref[1 - l])
        warm = mix(air_ref[2 + l], air_ref[3 - l])
        mixed_ref[8 * l : 8 * l + 8, :] = vapour[4:12, :128]
        mixed_ref[16 + 8 * l : 24 + 8 * l, :] = warm[4:12, :128]
        humid = moisture_excess(vapour, warm)
        humid_ref[8 * l : 8 * l + 8, :] = humid[0:8, :]
        moved.append(stencil(humid))

    for f in range(FIELDS):
        for r in range(8):
            halo_ref[f, pl.ds(r, 8, stride=8), :] = west_ref[pl.ds(16 * f + r % 2, 8, stride=2), :]
    windows = [
        [
            jnp.concatenate([moved[0][a][b][3:4, :], moved[1][a][b][3:4, :]] * 4, 0)
            for b in range(3)
        ]
        for a in range(3)
    ]
    tiles = [[halo_ref[f, 8 * k : 8 * k + 8, :] for k in range(SD)] for f in range(5)]
    order = [halo_ref[5, 8 * k : 8 * k + 8, :].astype(I32) for k in range(SD)]
    halo_radius, halo_mult, outer = droplets(windows, *tiles, order)
    for k in range(SD):
        table_ref[0, 8 * k : 8 * k + 8, :] = halo_radius[k]
        table_ref[1, 8 * k : 8 * k + 8, :] = halo_mult[k]
    face_records(
        west_ref[X_LIST : X_LIST + 8, :], 1, 0, table_ref, halo_ref, record_ref, box_ref
    )

    from_west = along_y(outer, 2)
    for l in range(2):
        windows = [[moved[l][a][b][4:12, :] for b in range(3)] for a in range(3)]
        tiles = [
            [ref[k * 16 + 8 * l : k * 16 + 8 * l + 8, :] for k in range(SD)]
            for ref in (sz_ref, wt_ref, dn_ref, ox_ref, oy_ref, pm_ref)
        ]
        radius, coalesced, deposit = droplets(windows, *tiles)
        for k in range(SD):
            rows = slice(k * 16 + 8 * l, k * 16 + 8 * l + 8)
            size_ref[rows, :] = radius[k]
            mult_ref[rows, :] = jnp.where(mask_ref[rows, :] > 0.5, 0.0, coalesced[k])
        own = [jnp.where(row8 < 6, along_y(deposit, a), 0.0) for a in range(3)]
        west_row = jnp.broadcast_to(from_west[l : l + 1, :], (8, 128))
        source_ref[8 * l : 8 * l + 8, :] = (
            own[1]
            + jnp.where(row8 == 0, west_row, shift(own[2], 1, 0))
            + jnp.where(row8 == 7, 0.0, shift(own[0], -1, 0))
        )


def east_kernel(
    q_ref, t_ref, sz_ref, wt_ref, dn_ref, ox_ref, oy_ref, pm_ref, mask_ref, rim_ref, west_ref,
    east_ref, early_size, early_mult, humid_ref, mixed_ref, source_ref, west_record, west_box,
    moist_out, warm_out, size_out, mult_out, record_out, box_out,
    moist_ref, warm_ref, size_ref, mult_ref, record_ref, box_ref,
    halo_ref, table_ref, air_ref, sems,
):
    leaving = [
        pltpu.make_async_copy(source, target, sems.at[n])
        for n, (source, target) in enumerate((
            (west_record, record_out.at[:, :, 0:1024]), (west_box, box_out.at[:, 0:1024]),
            (size_ref, size_out), (mult_ref, mult_out),
            (record_ref, record_out.at[:, :, 1024:2176]), (box_ref, box_out.at[:, 1024:2176]),
            (moist_ref, moist_out), (warm_ref, warm_out),
        ))
    ]
    leaving[0].start()
    leaving[1].start()
    lane = lanes_of((8, 128))
    lane1 = lanes_of((1, 128))
    row8 = rows_of((8, 128))
    slot = lane % 16
    for a, own_ref in enumerate((q_ref, t_ref)):
        for l in range(2):
            g = 2 * a + l
            row = X_AIR + 3 * g
            far = X_EXT + 3 * g
            air_ref[g, 0:5, :128] = own_ref[8 * l + 3 : 8 * l + 8, :]
            air_ref[g, 0:5, 128:] = rim_ref[R_EXT + 8 * g + 3 : R_EXT + 8 * g + 8, :]
            air_ref[g, 5:8, :128] = east_ref[row : row + 3, :]
            air_ref[g, 5:8, 128:] = east_ref[far : far + 3, :]
    mixed = []
    moved = []
    near = []
    for l in range(2):
        vapour = mix(air_ref[l], air_ref[1 - l])
        warm = mix(air_ref[2 + l], air_ref[3 - l])
        mixed.append((shift(vapour[:, :128], 3, 0), shift(warm[:, :128], 3, 0)))
        humid = moisture_excess(vapour, warm)
        moved.append(stencil(humid))
        near.append((humid_ref[8 * l : 8 * l + 8, :], shift(humid, -1, 0)))
    south = lane < 32
    upper = lane % 32 >= 16
    rim = []
    for b in range(3):
        spread = []
        for tile in range(2):
            levels = []
            for l in range(2):
                main, beside = near[l][tile][:, :128], near[l][tile][:, 128:]
                if b == 1:
                    got = jnp.take_along_axis(beside, jnp.where(south, 127, 0), axis=1)
                else:
                    place = jnp.where(south, 126, 127) if b == 0 else jnp.where(south, 0, 1)
                    first, second = (beside, main) if b == 0 else (main, beside)
                    got = jnp.where(
                        south,
                        jnp.take_along_axis(first, place, axis=1),
                        jnp.take_along_axis(second, place, axis=1),
                    )
                levels.append(got)
            spread.append(jnp.where(upper, levels[1], levels[0]))
        lines = []
        for a in range(3):
            wanted = slot + (a - 1)
            both = jnp.where(row8 == wanted, spread[0], 0.0)
            both = both + jnp.where(row8 + 8 == wanted, spread[1], 0.0)
            lines.append(jnp.sum(both, axis=0, keepdims=True))
        rim.append(lines)

    beyond = []
    for f, own_ref in enumerate((sz_ref, wt_ref, dn_ref, ox_ref, oy_ref, pm_ref)):
        line = jnp.where(
            slot == 3,
            shift(west_ref[X_CORNER : X_CORNER + 8, :], 3 - f, 1),
            jnp.where(
                slot == 12,
                shift(east_ref[X_CORNER : X_CORNER + 8, :], 12 - f, 1),
                rim_ref[8 * f : 8 * f + 8, :],
            ),
        )
        line = jnp.where((lane < 64) & (slot >= 3) & (slot <= 12), line, 0.0 if f == 5 else 0.5)
        beyond.append(line)
        for l in range(2):
            for n, i in enumerate((6, 7)):
                own = own_ref[pl.ds(8 * l + i, 8, stride=16), :]
                halo_ref[f, pl.ds(2 * n + l, 8, stride=8), :] = own.astype(F32)
            east = east_ref[pl.ds(16 * f + l, 8, stride=2), :]
            halo_ref[f, pl.ds(4 + l, 8, stride=8), :] = east
            halo_ref[f, pl.ds(6 + l, 8, stride=8), :] = line
    windows = [
        [
            jnp.concatenate(
                [moved[l][a][b][r : r + 1, :] for r in (3, 4, 5) for l in range(2)]
                + [rim[b][a]] * 2,
                0,
            )
            for b in range(3)
        ]
        for a in range(3)
    ]
    tiles = [[halo_ref[f, 8 * k : 8 * k + 8, :] for k in range(SD)] for f in range(5)]
    order = [halo_ref[5, 8 * k : 8 * k + 8, :].astype(I32) for k in range(SD)]
    radius, coalesced, outer = droplets(windows, *tiles, order)
    for k in range(SD):
        table_ref[0, 8 * k : 8 * k + 8, :] = radius[k]
        table_ref[1, 8 * k : 8 * k + 8, :] = coalesced[k]

    size_ref[...] = early_size[...]
    mult_ref[...] = early_mult[...]
    for l in range(2):
        for n, i in enumerate((6, 7)):
            rows = pl.ds(8 * l + i, 8, stride=16)
            at = pl.ds(2 * n + l, 8, stride=8)
            size_ref[rows, :] = table_ref[0, at, :]
            mult_ref[rows, :] = jnp.where(mask_ref[rows, :] > 0.5, 0.0, table_ref[1, at, :])
    leaving[2].start()
    leaving[3].start()

    face_records(
        east_ref[X_LIST : X_LIST + 8, :], -1, 4, table_ref, halo_ref, record_ref, box_ref
    )
    diagonal = lane >= 96
    by_west = diagonal & (lane % 16 < 8)
    entry = jnp.where(
        by_west,
        west_ref[X_CORNER : X_CORNER + 8, :],
        jnp.where(diagonal, east_ref[X_CORNER : X_CORNER + 8, :], rim_ref[G_LIST:G_ROWS, :]),
    ).astype(I32)
    live = entry >= 0
    north_side = ((lane >= 48) & (lane < 96)) | (lane >= 112)
    column = entry & 127
    i = (entry >> 7) & 7
    level = (entry >> 10) & 1
    place = i + 4 + jnp.where(diagonal, jnp.where(by_west, -8, 8), 0)
    at = (jnp.where(north_side, 32, 0) + level * 16 + place) & 127
    mine = live & ((entry >> 11) == row8)
    dx = jnp.where(diagonal, jnp.where(by_west, 1, -1), 0)
    dy = jnp.where(north_side, -1, 1)
    box = (level * 8 + ((i + dx) & 7)) * 128 + ((column + dy) & 127)
    box_ref[0:1, 1024:1152] = jnp.where(live, box, -1)[0:1, :]
    for n in range(5):
        table = table_ref[n, pl.ds(6, 8, stride=8), :] if n < 2 else beyond[n]
        got = jnp.take_along_axis(table, at, axis=1)
        line = jnp.sum(jnp.where(mine, got, 0.0), axis=0, keepdims=True)
        record_ref[n, 0:1, 1024:1152] = line
    leaving[4].start()
    leaving[5].start()

    down, level_row, up = (along_y(outer, a) for a in range(3))
    rim_line = [jnp.where(lane1 < 32, outer[a][2][6:7, :], outer[a][0][6:7, :]) for a in range(3)]
    rim_line = [jnp.broadcast_to(line, (8, 128)) for line in rim_line]
    for l in range(2):
        extra = (
            down[l : l + 1, :],
            level_row[l : l + 1, :] + down[2 + l : 3 + l, :],
            up[l : l + 1, :] + level_row[2 + l : 3 + l, :] + down[4 + l : 5 + l, :],
        )
        added = jnp.zeros((8, 128), F32)
        for r, line in zip((5, 6, 7), extra):
            added = jnp.where(row8 == r, jnp.broadcast_to(line, (8, 128)), added)
        rows = slice(8 * l, 8 * l + 8)
        source = source_ref[rows, :] + added
        for side, j in enumerate((0, 127)):
            place = side * 32 + l * 16 + 4 + row8
            part = jnp.where(lane == place - 1, rim_line[2], 0.0)
            part = jnp.where(lane == place, rim_line[1], part)
            part = jnp.where(lane == place + 1, rim_line[0], part)
            part = jnp.sum(part, axis=1, keepdims=True)
            source = source + jnp.where(lane == j, part, 0.0)
        vapour = jnp.where(row8 < 4, mixed_ref[rows, :], mixed[l][0])
        warm = jnp.where(row8 < 4, mixed_ref[16 + 8 * l : 24 + 8 * l, :], mixed[l][1])
        moist_ref[rows, :] = vapour - VAPOUR_PER_SOURCE * source
        warm_ref[rows, :] = warm + WARMING_FACTOR * source
    leaving[6].start()
    leaving[7].start()
    for copy in leaving:
        copy.wait()


def call(kernel, outs, args, scratch=(), space=pltpu.VMEM):
    return pl.pallas_call(
        kernel,
        out_shape=outs,
        in_specs=[pl.BlockSpec(memory_space=pltpu.VMEM)] * len(args),
        out_specs=jax.tree.map(lambda _: pl.BlockSpec(memory_space=space), outs),
        scratch_shapes=list(scratch),
        compiler_params=pltpu.CompilerParams(vmem_limit_bytes=8 << 20),
        cost_estimate=pl.CostEstimate(flops=1 << 20, bytes_accessed=1 << 18, transcendentals=0),
    )(*args)


def ring(axis, step):
    count = lax.axis_size(axis)
    return [(i, (i + step) % count) for i in range(count)]


def swaps(axis, first):
    count = lax.axis_size(axis)
    pairs = [(i % count, (i + 1) % count) for i in range(first, count, 2)]
    return pairs + [(target, source) for source, target in pairs]


def per_device(
    moisture_ratio,
    kelvin_warmth,
    droplet_size_micron,
    weighting_factor,
    dry_nucleus_size,
    fractional_offset_east,
    fractional_offset_north,
    encounter_permutation,
    departing_eastwest_lists,
    departing_northsouth_lists,
    departing_diagonal_lists,
):
    def f32(*shape):
        return jax.ShapeDtypeStruct(shape, F32)

    air = (moisture_ratio.reshape(16, 128), kelvin_warmth.reshape(16, 128))
    drops = tuple(
        x.reshape(128, 128)
        for x in (
            droplet_size_micron,
            weighting_factor,
            dry_nucleus_size,
            fractional_offset_east,
            fractional_offset_north,
            encounter_permutation,
        )
    )
    given = (*air, *drops, departing_eastwest_lists)
    short = (departing_northsouth_lists, departing_diagonal_lists)
    *given, east_west, to_gy = pl.pallas_call(
        pack_gy_kernel,
        out_shape=(*(pltpu.VMEM(x.shape, x.dtype) for x in given), pltpu.VMEM((G_ROWS, 128), F32)),
        in_specs=[pl.BlockSpec(memory_space=pltpu.HBM)] * 11,
        out_specs=(pl.BlockSpec(memory_space=pltpu.VMEM),) * 10,
        scratch_shapes=(
            *(pltpu.VMEM(x.shape, x.dtype) for x in short),
            pltpu.VMEM((8, 128), F32),
            pltpu.SemaphoreType.DMA((11,)),
        ),
        compiler_params=pltpu.CompilerParams(vmem_limit_bytes=8 << 20),
        cost_estimate=pl.CostEstimate(flops=1 << 20, bytes_accessed=1 << 18, transcendentals=0),
    )(*(pltpu.with_memory_space_constraint(x, pltpu.HBM) for x in (*given, *short)))
    far = lax.ppermute(to_gy, "gy", swaps("gy", 1))
    count = lax.axis_size("gy")
    near = lax.all_gather(to_gy, "gy", axis_index_groups=[[i, i + 1] for i in range(0, count, 2)])
    departed = call(departed_kernel, f32(128, 128), (east_west, to_gy))
    to_east, to_west, rim = call(
        pack_gx_kernel,
        (f32(X_ROWS, 128), f32(X_ROWS, 128), f32(R_ROWS, 128)),
        (*given, east_west, near, far),
    )
    from_west = lax.ppermute(to_east, "gx", ring("gx", 1))
    from_east = lax.ppermute(to_west, "gx", ring("gx", -1))
    scratch = (pltpu.VMEM((FIELDS, 64, 128), F32), pltpu.VMEM((2, 64, 128), F32))
    early = call(
        west_kernel,
        (
            pltpu.VMEM((128, 128), F32),
            pltpu.VMEM((128, 128), F32),
            pltpu.VMEM((16, 256), F32),
            pltpu.VMEM((32, 128), F32),
            pltpu.VMEM((16, 128), F32),
            pltpu.VMEM((5, 1, 1024), F32),
            pltpu.VMEM((1, 1024), I32),
        ),
        (*given, departed, rim, from_west),
        scratch=(*scratch, pltpu.VMEM((4, 16, 256), F32)),
    )
    moist, warm, size, mult, records, box = call(
        east_kernel,
        (
            f32(16, 128),
            f32(16, 128),
            f32(128, 128),
            f32(128, 128),
            f32(5, 1, 2176),
            jax.ShapeDtypeStruct((1, 2176), I32),
        ),
        (*given, departed, rim, from_west, from_east, *early),
        scratch=(
            pltpu.VMEM((16, 128), F32),
            pltpu.VMEM((16, 128), F32),
            pltpu.VMEM((128, 128), F32),
            pltpu.VMEM((128, 128), F32),
            pltpu.VMEM((5, 1, 1152), F32),
            pltpu.VMEM((1, 1152), I32),
            *scratch,
            pltpu.VMEM((4, 8, 256), F32),
            pltpu.SemaphoreType.DMA((8,)),
        ),
        space=pltpu.HBM,
    )
    return (
        moist.reshape(moisture_ratio.shape),
        warm.reshape(kelvin_warmth.shape),
        size.reshape(droplet_size_micron.shape),
        mult.reshape(weighting_factor.shape),
        records,
        box,
    )


def solution(mesh):
    cells = P(None, "gx", "gy")
    drop = P(None, None, "gx", "gy")
    lists = P("gx", None, "gy")
    return jax.shard_map(
        per_device,
        mesh=mesh,
        in_specs=(cells,) * 2 + (drop,) * 6 + (lists,) * 3,
        out_specs=(cells, cells, drop, drop, P(None, "gx", "gy"), P("gx", "gy")),
        check_vma=False,
    )
```

```python
import jax
import jax.numpy as jnp
from jax import lax
from jax.experimental import pallas as pl
from jax.experimental.pallas import tpu as pltpu
from jax.sharding import PartitionSpec as P


NEWTON = 4
MIX_HORIZONTAL = 0.2
MIX_VERTICAL = 0.05
EXCESS_FACTOR = 4.2222
CURVATURE = 0.0012
KAPPA_SOLUTE = 0.6
GROWTH_STEP = 200.0
COLLIDE_RATE = 4e-07
VAPOUR_PER_SOURCE = 0.001
WARMING_FACTOR = 0.00249

F32 = jnp.float32
I32 = jnp.int32
SD = 8
FIELDS = 6

G_LIST = 8 * FIELDS
G_ROWS = G_LIST + 8
R_EXT = G_ROWS
R_ROWS = R_EXT + 32
X_AIR = 16 * FIELDS
X_EXT = X_AIR + 12
X_CORNER = X_EXT + 12
X_LIST = X_CORNER + 8
X_ROWS = X_LIST + 8


def lanes_of(shape):
    return lax.broadcasted_iota(I32, shape, len(shape) - 1)


def shift(x, amount, axis):
    return pltpu.roll(x, amount % x.shape[axis], axis)


def rows_of(shape):
    return lax.broadcasted_iota(I32, shape, len(shape) - 2)


def pack_gy_kernel(*refs):
    given, kept = refs[:11], refs[11:20]
    g_ref, side_ref, corner_ref, line_ref, sems = refs[20:]
    copies = [
        pltpu.make_async_copy(source, target, sems.at[n])
        for n, (source, target) in enumerate(zip(given, (*kept, side_ref, corner_ref)))
    ]
    for copy in copies:
        copy.start()
    for copy in copies:
        copy.wait()
    line_ref[0:2, 0:48] = side_ref[0].astype(F32)
    line_ref[2:6, 0:8] = corner_ref[0].astype(F32)
    small = line_ref[0:1, :]
    lane1 = lanes_of((1, 128))
    for row, start in ((1, 48), (2, 96), (4, 104), (3, 112), (5, 120)):
        small = jnp.where(lane1 < start, small, pltpu.roll(line_ref[row : row + 1, :], start, 1))
    g_ref[G_LIST:G_ROWS, :] = jnp.broadcast_to(small, (8, 128))
    lane = lanes_of((8, 128))
    first = lane < 32
    low_level = lane % 32 < 16
    for f in range(FIELDS):
        ref = kept[2 + f]
        parts = [ref[k * 16 : k * 16 + 16, :] for k in (0, 7, 6, 5, 4, 3, 2, 1)]
        block = jnp.concatenate(parts, 0)
        if f == 5:
            block = block.astype(F32)
        turned = jnp.transpose(block)
        out = []
        for row in (127, 0):
            line = jnp.broadcast_to(turned[row : row + 1, :], (8, 128))
            lev0 = pltpu.roll(line, 4, 1, stride=16, stride_axis=0)
            lev1 = pltpu.roll(line, 12, 1, stride=16, stride_axis=0)
            out.append(jnp.where(low_level, lev0, lev1))
        out[1] = shift(out[1], -2, 0)
        block = jnp.where(first, out[0], out[1])
        if f < 4:
            air = kept[f // 2][8 * (f % 2) : 8 * (f % 2) + 8, :]
            block = jnp.where(lane < 64, block, pltpu.roll(air, 67, 1))
        g_ref[f * 8 : f * 8 + 8, :] = block


def pack_gx_kernel(
    q_ref, t_ref, sz_ref, wt_ref, dn_ref, ox_ref, oy_ref, pm_ref, list_ref, near_ref, far_ref,
    east_ref, west_ref, rim_ref,
):
    even = lax.axis_index("gy") % 2 == 0
    lane = lanes_of((8, 128))
    slot = lane % 16
    from_near = (((lane >= 32) & (lane < 64)) | (lane >= 67)) == even
    blocks = []
    for f in range(FIELDS):
        rows = slice(8 * f, 8 * f + 8)
        near = jnp.where(even, near_ref[1, rows, :], near_ref[0, rows, :])
        merged = jnp.where(from_near, near, far_ref[rows, :])
        rim_ref[rows, :] = merged
        blocks.append(merged)
    from_near = (((lane >= 48) & (lane < 96)) | (lane >= 112)) == even
    near = jnp.where(even, near_ref[1, G_LIST:G_ROWS, :], near_ref[0, G_LIST:G_ROWS, :])
    small = jnp.where(from_near, near, far_ref[G_LIST:G_ROWS, :])
    rim_ref[G_LIST:G_ROWS, :] = small
    ext = [shift(blocks[g], -67, 1) for g in range(4)]
    for g in range(4):
        rim_ref[R_EXT + 8 * g : R_EXT + 8 * g + 8, :] = ext[g]
    drops = (sz_ref, wt_ref, dn_ref, ox_ref, oy_ref, pm_ref)
    for side, (out_ref, i, row) in enumerate(((east_ref, 7, 5), (west_ref, 0, 0))):
        for f, ref in enumerate(drops):
            face = ref[pl.ds(i, 16, stride=8), :]
            if f == 5:
                face = face.astype(F32)
            out_ref[16 * f : 16 * f + 16, :] = face
        for g in range(4):
            ref = (q_ref, t_ref)[g // 2]
            at = 8 * (g % 2) + row
            out_ref[X_AIR + 3 * g : X_AIR + 3 * g + 3, :] = ref[at : at + 3, :]
            out_ref[X_EXT + 3 * g : X_EXT + 3 * g + 3, :] = ext[g][row : row + 3, :]
        corner = small
        for f in range(FIELDS):
            here = (lane < 64) & (slot == f)
            corner = jnp.where(here, shift(blocks[f], f - 4 - i, 1), corner)
        out_ref[X_CORNER : X_CORNER + 8, :] = corner
        for c in range(8):
            piece = list_ref[0, side : side + 1, 128 * c : 128 * c + 128]
            out_ref[X_LIST + c : X_LIST + c + 1, :] = piece.astype(F32)


def one_hot(values, rows):
    shape = (rows, values.shape[1])
    hit = jnp.broadcast_to(values, shape) == rows_of(shape)
    return jnp.where(hit, 1.0, 0.0).astype(jnp.bfloat16)


def counts(rows, columns):
    return lax.dot_general(rows, columns, (((1,), (1,)), ((), ())), preferred_element_type=F32)


def departed_kernel(list_ref, g_ref, mask_ref):
    entry = g_ref[G_LIST : G_LIST + 1, :].astype(I32)
    mask_ref[...] = counts(one_hot(entry >> 7, 128), one_hot(entry & 127, 128))
    for side, i in ((0, 7), (1, 0)):
        entry = list_ref[0, side : side + 1, :]
        found = counts(one_hot(entry >> 10, 16), one_hot(entry & 127, 128))
        rows = pl.ds(i, 16, stride=8)
        mask_ref[rows, :] = mask_ref[rows, :] + found


def grow(size, dry, forcing):
    initial = size * size
    lowest = dry * dry
    solute = KAPPA_SOLUTE * lowest * dry
    target = initial + GROWTH_STEP * forcing
    upper = (2.5 * GROWTH_STEP) * solute
    lower = (1.5 * GROWTH_STEP) * solute
    wetted = initial
    for _ in range(NEWTON):
        power = wetted * wetted * (wetted * lax.rsqrt(wetted))
        wetted = jnp.maximum((target * power + upper * wetted) / (power + lower), lowest)
    return wetted


def pick(values, bits):
    low, mid, high = bits
    a = [jnp.where(low, values[2 * n + 1], values[2 * n]) for n in range(4)]
    b = [jnp.where(mid, a[2 * n + 1], a[2 * n]) for n in range(2)]
    return jnp.where(high, b[1], b[0])


def coalesce(grown, mult, order):
    bits = [((o & 1) == 1, (o & 2) == 2, o >= 4) for o in order]
    changed = []
    for pair in range(SD // 2):
        first, second = order[2 * pair], order[2 * pair + 1]
        p, q = bits[2 * pair], bits[2 * pair + 1]
        r1, r2 = pick(grown, p), pick(grown, q)
        m1, m2 = pick(mult, p), pick(mult, q)
        big = m1 >= m2
        hr, lr = jnp.where(big, r1, r2), jnp.where(big, r2, r1)
        hm, lm = jnp.where(big, m1, m2), jnp.where(big, m2, m1)
        total = r1 + r2
        rate = COLLIDE_RATE * hm * (total * total) * jnp.abs(r1 * r1 - r2 * r2)
        chance = 1.0 - jnp.exp(-rate)
        volume = lr * lr * lr + chance * (hr * hr * hr)
        merged = jnp.exp2(jnp.log2(volume) * (1.0 / 3.0))
        reduced = hm - chance * lm
        high, low = jnp.where(big, first, second), jnp.where(big, second, first)
        changed.append((high, low, merged, reduced))
    out_radius, out_mult = [], []
    for target in range(SD):
        r, m = grown[target], mult[target]
        for high, low, merged, reduced in changed:
            r = jnp.where(low == target, merged, r)
            m = jnp.where(high == target, reduced, m)
        out_radius.append(r)
        out_mult.append(m)
    return out_radius, out_mult


def droplets(windows, size, mult, dry, east, north, order):
    lines = [(w[1], w[0] - w[1], w[2] - w[1]) for w in windows]
    middle = lines[1]
    below = [x - y for x, y in zip(lines[0], middle)]
    above = [x - y for x, y in zip(lines[2], middle)]
    total = [[None] * 3 for _ in range(3)]
    grown = []
    for k in range(SD):
        dx, dy = east[k] - 0.5, north[k] - 0.5
        ahead_x, ahead_y = dx > 0.0, dy > 0.0
        along, across = jnp.abs(dx), jnp.abs(dy)
        outer = [jnp.where(ahead_x, x, y) for x, y in zip(above, below)]
        forcing = middle[0] + across * jnp.where(ahead_y, middle[2], middle[1])
        forcing = forcing + along * (outer[0] + across * jnp.where(ahead_y, outer[2], outer[1]))
        forcing = forcing - CURVATURE / size[k]
        wetted = grow(size[k], dry[k], forcing)
        radius = wetted * lax.rsqrt(wetted)
        condensed = mult[k] * (wetted * radius - size[k] * size[k] * size[k])
        up_x, up_y = jnp.maximum(dx, 0.0), jnp.maximum(dy, 0.0)
        down_x, down_y = up_x - dx, up_y - dy
        row = (condensed, condensed * down_y, condensed * up_y)
        for a, factor in enumerate((None, down_x, up_x)):
            for b in range(3):
                term = row[b] if factor is None else row[b] * factor
                total[a][b] = term if k == 0 else total[a][b] + term
        grown.append(radius)
    total = [(t[1], t[0] - t[1] - t[2], t[2]) for t in total]
    deposit = [
        total[1],
        tuple(x - y - z for x, y, z in zip(*total)),
        total[2],
    ]
    radius, coalesced = coalesce(grown, mult, order)
    return radius, coalesced, deposit


def mix(x, other):
    across = shift(x, 1, 0) + shift(x, -1, 0) + shift(x, 1, 1) + shift(x, -1, 1) - 4.0 * x
    return x + MIX_HORIZONTAL * across + MIX_VERTICAL * (other + x - 2.0 * x)


def moisture_excess(vapour, warm):
    most = EXCESS_FACTOR * jnp.exp(17.27 * (warm - 273.15) / (warm - 35.86))
    return vapour / most - 1.0


def stencil(humid):
    columns = [shift(humid, 1, 1)[:, :128], humid[:, :128], shift(humid, -1, 1)[:, :128]]
    return [[shift(c, 1, 0) for c in columns], columns, [shift(c, -1, 0) for c in columns]]


def rim_rows(lower, upper, first):
    lane = lanes_of((8, 128))
    row = rows_of((8, 128)) + first
    slot = lane % 16
    south = lane < 32
    rim = []
    for b in range(3):
        levels = []
        for humid in (lower, upper):
            main, beside = humid[:, :128], humid[:, 128:]
            if b == 1:
                got = jnp.take_along_axis(beside, jnp.where(south, 127, 0), axis=1)
            else:
                place = jnp.where(south, 126, 127) if b == 0 else jnp.where(south, 0, 1)
                outer, inner = (beside, main) if b == 0 else (main, beside)
                got = jnp.where(
                    south,
                    jnp.take_along_axis(outer, place, axis=1),
                    jnp.take_along_axis(inner, place, axis=1),
                )
            levels.append(got)
        spread = jnp.where(lane % 32 >= 16, levels[1], levels[0])
        rim.append([
            jnp.sum(jnp.where(row == slot + (a - 1), spread, 0.0), axis=0, keepdims=True)
            for a in range(3)
        ])
    return rim


def along_y(d, a):
    lane = lanes_of((8, 128))
    return (
        d[a][1]
        + jnp.where(lane == 0, 0.0, shift(d[a][2], 1, 1))
        + jnp.where(lane == 127, 0.0, shift(d[a][0], -1, 1))
    )


def face_records(list_rows, step, first_row, table_ref, halo_ref, record_ref, box_ref):
    entry = list_rows.astype(I32)
    live = entry >= 0
    column = entry & 127
    group = entry >> 10
    picked = [jnp.zeros((8, 128), F32) for _ in range(5)]
    for k in range(SD):
        for l in range(2):
            here = live & (group == 2 * k + l)
            r = 8 * k + first_row + l
            for n in range(5):
                src = table_ref if n < 2 else halo_ref
                line = jnp.broadcast_to(src[n, r : r + 1, :], (8, 128))
                got = jnp.take_along_axis(line, column, axis=1)
                picked[n] = jnp.where(here, got, picked[n])
    box = (((entry >> 10) & 1) * 8 + (((entry >> 7) + step) & 7)) * 128 + column
    box = jnp.where(live, box, -1)
    for c in range(8):
        lanes = slice(c * 128, c * 128 + 128)
        for n in range(5):
            record_ref[n, 0:1, lanes] = picked[n][c : c + 1, :]
        box_ref[0:1, lanes] = box[c : c + 1, :]


def west_kernel(
    q_ref, t_ref, sz_ref, wt_ref, dn_ref, ox_ref, oy_ref, pm_ref, mask_ref, rim_ref, west_ref,
    size_ref, mult_ref, share_ref, mixed_ref, source_ref, record_ref, box_ref, line_ref,
    halo_ref, table_ref, air_ref,
):
    row8 = rows_of((8, 128))
    for a, own_ref in enumerate((q_ref, t_ref)):
        for l in range(2):
            g = 2 * a + l
            row = X_AIR + 3 * g
            far = X_EXT + 3 * g
            air_ref[g, 4:12, :128] = own_ref[8 * l : 8 * l + 8, :]
            air_ref[g, 4:12, 128:] = rim_ref[R_EXT + 8 * g : R_EXT + 8 * g + 8, :]
            air_ref[g, 1:4, :128] = west_ref[row : row + 3, :]
            air_ref[g, 1:4, 128:] = west_ref[far : far + 3, :]
    moved = []
    humids = []
    for l in range(2):
        vapour = mix(air_ref[l], air_ref[1 - l])
        warm = mix(air_ref[2 + l], air_ref[3 - l])
        mixed_ref[8 * l : 8 * l + 8, :] = vapour[4:12, :128]
        mixed_ref[16 + 8 * l : 24 + 8 * l, :] = warm[4:12, :128]
        humid = moisture_excess(vapour, warm)
        humids.append(humid[0:8, :])
        moved.append(stencil(humid))
    share = rim_rows(*humids, 0)
    for b in range(3):
        for a in range(3):
            share_ref[3 * b + a : 3 * b + a + 1, :] = share[b][a]

    lane = lanes_of((8, 128))
    slot = lane % 16
    for f in range(FIELDS):
        line = jnp.where(
            slot == 3,
            shift(west_ref[X_CORNER : X_CORNER + 8, :], 3 - f, 1),
            rim_ref[8 * f : 8 * f + 8, :],
        )
        line = jnp.where((lane < 64) & (slot >= 3) & (slot < 12), line, 0.0 if f == 5 else 0.5)
        line_ref[8 * f : 8 * f + 8, :] = line
        for r in range(8):
            halo_ref[f, pl.ds(r, 8, stride=8), :] = west_ref[pl.ds(16 * f + r % 2, 8, stride=2), :]
    windows = [
        [
            jnp.concatenate([moved[0][a][b][3:4, :], moved[1][a][b][3:4, :]] * 4, 0)
            for b in range(3)
        ]
        for a in range(3)
    ]
    tiles = [[halo_ref[f, 8 * k : 8 * k + 8, :] for k in range(SD)] for f in range(5)]
    order = [halo_ref[5, 8 * k : 8 * k + 8, :].astype(I32) for k in range(SD)]
    halo_radius, halo_mult, outer = droplets(windows, *tiles, order)
    for k in range(SD):
        table_ref[0, 8 * k : 8 * k + 8, :] = halo_radius[k]
        table_ref[1, 8 * k : 8 * k + 8, :] = halo_mult[k]
    face_records(
        west_ref[X_LIST : X_LIST + 8, :], 1, 0, table_ref, halo_ref, record_ref, box_ref
    )

    from_west = along_y(outer, 2)
    for l in range(2):
        windows = [[moved[l][a][b][4:12, :] for b in range(3)] for a in range(3)]
        tiles = [
            [ref[k * 16 + 8 * l : k * 16 + 8 * l + 8, :] for k in range(SD)]
            for ref in (sz_ref, wt_ref, dn_ref, ox_ref, oy_ref, pm_ref)
        ]
        radius, coalesced, deposit = droplets(windows, *tiles)
        for k in range(SD):
            rows = slice(k * 16 + 8 * l, k * 16 + 8 * l + 8)
            size_ref[rows, :] = radius[k]
            mult_ref[rows, :] = jnp.where(mask_ref[rows, :] > 0.5, 0.0, coalesced[k])
        own = [jnp.where(row8 < 6, along_y(deposit, a), 0.0) for a in range(3)]
        west_row = jnp.broadcast_to(from_west[l : l + 1, :], (8, 128))
        source_ref[8 * l : 8 * l + 8, :] = (
            own[1]
            + jnp.where(row8 == 0, west_row, shift(own[2], 1, 0))
            + jnp.where(row8 == 7, 0.0, shift(own[0], -1, 0))
        )


def east_kernel(
    q_ref, t_ref, sz_ref, wt_ref, dn_ref, ox_ref, oy_ref, pm_ref, mask_ref, rim_ref, west_ref,
    east_ref, early_size, early_mult, share_ref, mixed_ref, source_ref, west_record, west_box, line_ref,
    moist_out, warm_out, size_out, mult_out, record_out, box_out,
    moist_ref, warm_ref, size_ref, mult_ref, record_ref, box_ref,
    halo_ref, table_ref, air_ref, sems,
):
    leaving = [
        pltpu.make_async_copy(source, target, sems.at[n])
        for n, (source, target) in enumerate((
            (west_record, record_out.at[:, :, 0:1024]), (west_box, box_out.at[:, 0:1024]),
            (size_ref, size_out), (mult_ref, mult_out),
            (record_ref, record_out.at[:, :, 1024:2176]), (box_ref, box_out.at[:, 1024:2176]),
            (moist_ref, moist_out), (warm_ref, warm_out),
        ))
    ]
    leaving[0].start()
    leaving[1].start()
    lane = lanes_of((8, 128))
    lane1 = lanes_of((1, 128))
    row8 = rows_of((8, 128))
    slot = lane % 16
    for a, own_ref in enumerate((q_ref, t_ref)):
        for l in range(2):
            g = 2 * a + l
            row = X_AIR + 3 * g
            far = X_EXT + 3 * g
            air_ref[g, 0:5, :128] = own_ref[8 * l + 3 : 8 * l + 8, :]
            air_ref[g, 0:5, 128:] = rim_ref[R_EXT + 8 * g + 3 : R_EXT + 8 * g + 8, :]
            air_ref[g, 5:8, :128] = east_ref[row : row + 3, :]
            air_ref[g, 5:8, 128:] = east_ref[far : far + 3, :]
    mixed = []
    moved = []
    near = []
    for l in range(2):
        vapour = mix(air_ref[l], air_ref[1 - l])
        warm = mix(air_ref[2 + l], air_ref[3 - l])
        mixed.append((shift(vapour[:, :128], 3, 0), shift(warm[:, :128], 3, 0)))
        humid = moisture_excess(vapour, warm)
        moved.append(stencil(humid))
        near.append(shift(humid, -1, 0))
    rim = rim_rows(*near, 8)
    for b in range(3):
        for a in range(3):
            rim[b][a] = rim[b][a] + share_ref[3 * b + a : 3 * b + a + 1, :]

    beyond = []
    for f, own_ref in enumerate((sz_ref, wt_ref, dn_ref, ox_ref, oy_ref, pm_ref)):
        line = jnp.where(
            (lane < 64) & (slot == 12),
            shift(east_ref[X_CORNER : X_CORNER + 8, :], 12 - f, 1),
            line_ref[8 * f : 8 * f + 8, :],
        )
        beyond.append(line)
        for l in range(2):
            for n, i in enumerate((6, 7)):
                own = own_ref[pl.ds(8 * l + i, 8, stride=16), :]
                halo_ref[f, pl.ds(2 * n + l, 8, stride=8), :] = own.astype(F32)
            east = east_ref[pl.ds(16 * f + l, 8, stride=2), :]
            halo_ref[f, pl.ds(4 + l, 8, stride=8), :] = east
            halo_ref[f, pl.ds(6 + l, 8, stride=8), :] = line
    windows = [
        [
            jnp.concatenate(
                [moved[l][a][b][r : r + 1, :] for r in (3, 4, 5) for l in range(2)]
                + [rim[b][a]] * 2,
                0,
            )
            for b in range(3)
        ]
        for a in range(3)
    ]
    tiles = [[halo_ref[f, 8 * k : 8 * k + 8, :] for k in range(SD)] for f in range(5)]
    order = [halo_ref[5, 8 * k : 8 * k + 8, :].astype(I32) for k in range(SD)]
    radius, coalesced, outer = droplets(windows, *tiles, order)
    for k in range(SD):
        table_ref[0, 8 * k : 8 * k + 8, :] = radius[k]
        table_ref[1, 8 * k : 8 * k + 8, :] = coalesced[k]

    down, level_row, up = (along_y(outer, a) for a in range(3))
    rim_line = [jnp.where(lane1 < 32, outer[a][2][6:7, :], outer[a][0][6:7, :]) for a in range(3)]
    rim_line = [jnp.broadcast_to(line, (8, 128)) for line in rim_line]
    for l in range(2):
        extra = (
            down[l : l + 1, :],
            level_row[l : l + 1, :] + down[2 + l : 3 + l, :],
            up[l : l + 1, :] + level_row[2 + l : 3 + l, :] + down[4 + l : 5 + l, :],
        )
        added = jnp.zeros((8, 128), F32)
        for r, line in zip((5, 6, 7), extra):
            added = jnp.where(row8 == r, jnp.broadcast_to(line, (8, 128)), added)
        rows = slice(8 * l, 8 * l + 8)
        source = source_ref[rows, :] + added
        for side, j in enumerate((0, 127)):
            place = side * 32 + l * 16 + 4 + row8
            part = jnp.where(lane == place - 1, rim_line[2], 0.0)
            part = jnp.where(lane == place, rim_line[1], part)
            part = jnp.where(lane == place + 1, rim_line[0], part)
            part = jnp.sum(part, axis=1, keepdims=True)
            source = source + jnp.where(lane == j, part, 0.0)
        vapour = jnp.where(row8 < 4, mixed_ref[rows, :], mixed[l][0])
        warm = jnp.where(row8 < 4, mixed_ref[16 + 8 * l : 24 + 8 * l, :], mixed[l][1])
        moist_ref[rows, :] = vapour - VAPOUR_PER_SOURCE * source
        warm_ref[rows, :] = warm + WARMING_FACTOR * source
    leaving[6].start()
    leaving[7].start()
    size_ref[...] = early_size[...]
    mult_ref[...] = early_mult[...]
    for l in range(2):
        for n, i in enumerate((6, 7)):
            rows = pl.ds(8 * l + i, 8, stride=16)
            at = pl.ds(2 * n + l, 8, stride=8)
            size_ref[rows, :] = table_ref[0, at, :]
            mult_ref[rows, :] = jnp.where(mask_ref[rows, :] > 0.5, 0.0, table_ref[1, at, :])
    leaving[2].start()
    leaving[3].start()

    diagonal = lane >= 96
    by_west = diagonal & (lane % 16 < 8)
    entry = jnp.where(
        by_west,
        west_ref[X_CORNER : X_CORNER + 8, :],
        jnp.where(diagonal, east_ref[X_CORNER : X_CORNER + 8, :], rim_ref[G_LIST:G_ROWS, :]),
    ).astype(I32)
    live = entry >= 0
    north_side = ((lane >= 48) & (lane < 96)) | (lane >= 112)
    column = entry & 127
    i = (entry >> 7) & 7
    level = (entry >> 10) & 1
    place = i + 4 + jnp.where(diagonal, jnp.where(by_west, -8, 8), 0)
    at = (jnp.where(north_side, 32, 0) + level * 16 + place) & 127
    mine = live & ((entry >> 11) == row8)
    dx = jnp.where(diagonal, jnp.where(by_west, 1, -1), 0)
    dy = jnp.where(north_side, -1, 1)
    box = (level * 8 + ((i + dx) & 7)) * 128 + ((column + dy) & 127)
    box_ref[0:1, 1024:1152] = jnp.where(live, box, -1)[0:1, :]
    for n in range(5):
        table = table_ref[n, pl.ds(6, 8, stride=8), :] if n < 2 else beyond[n]
        got = jnp.take_along_axis(table, at, axis=1)
        line = jnp.sum(jnp.where(mine, got, 0.0), axis=0, keepdims=True)
        record_ref[n, 0:1, 1024:1152] = line
    face_records(
        east_ref[X_LIST : X_LIST + 8, :], -1, 4, table_ref, halo_ref, record_ref, box_ref
    )
    leaving[4].start()
    leaving[5].start()

    for copy in leaving:
        copy.wait()


def call(kernel, outs, args, scratch=(), space=pltpu.VMEM):
    return pl.pallas_call(
        kernel,
        out_shape=outs,
        in_specs=[pl.BlockSpec(memory_space=pltpu.VMEM)] * len(args),
        out_specs=jax.tree.map(lambda _: pl.BlockSpec(memory_space=space), outs),
        scratch_shapes=list(scratch),
        compiler_params=pltpu.CompilerParams(vmem_limit_bytes=8 << 20),
        cost_estimate=pl.CostEstimate(flops=1 << 20, bytes_accessed=1 << 18, transcendentals=0),
    )(*args)


def ring(axis, step):
    count = lax.axis_size(axis)
    return [(i, (i + step) % count) for i in range(count)]


def swaps(axis, first):
    count = lax.axis_size(axis)
    pairs = [(i % count, (i + 1) % count) for i in range(first, count, 2)]
    return pairs + [(target, source) for source, target in pairs]


def per_device(
    moisture_ratio,
    kelvin_warmth,
    droplet_size_micron,
    weighting_factor,
    dry_nucleus_size,
    fractional_offset_east,
    fractional_offset_north,
    encounter_permutation,
    departing_eastwest_lists,
    departing_northsouth_lists,
    departing_diagonal_lists,
):
    def f32(*shape):
        return jax.ShapeDtypeStruct(shape, F32)

    air = (moisture_ratio.reshape(16, 128), kelvin_warmth.reshape(16, 128))
    drops = tuple(
        x.reshape(128, 128)
        for x in (
            droplet_size_micron,
            weighting_factor,
            dry_nucleus_size,
            fractional_offset_east,
            fractional_offset_north,
            encounter_permutation,
        )
    )
    given = (*air, *drops, departing_eastwest_lists)
    short = (departing_northsouth_lists, departing_diagonal_lists)
    *given, east_west, to_gy = pl.pallas_call(
        pack_gy_kernel,
        out_shape=(*(pltpu.VMEM(x.shape, x.dtype) for x in given), pltpu.VMEM((G_ROWS, 128), F32)),
        in_specs=[pl.BlockSpec(memory_space=pltpu.HBM)] * 11,
        out_specs=(pl.BlockSpec(memory_space=pltpu.VMEM),) * 10,
        scratch_shapes=(
            *(pltpu.VMEM(x.shape, x.dtype) for x in short),
            pltpu.VMEM((8, 128), F32),
            pltpu.SemaphoreType.DMA((11,)),
        ),
        compiler_params=pltpu.CompilerParams(vmem_limit_bytes=8 << 20),
        cost_estimate=pl.CostEstimate(flops=1 << 20, bytes_accessed=1 << 18, transcendentals=0),
    )(*(pltpu.with_memory_space_constraint(x, pltpu.HBM) for x in (*given, *short)))
    far = lax.ppermute(to_gy, "gy", swaps("gy", 1))
    count = lax.axis_size("gy")
    near = lax.all_gather(to_gy, "gy", axis_index_groups=[[i, i + 1] for i in range(0, count, 2)])
    departed = call(departed_kernel, f32(128, 128), (east_west, to_gy))
    to_east, to_west, rim = call(
        pack_gx_kernel,
        (f32(X_ROWS, 128), f32(X_ROWS, 128), f32(R_ROWS, 128)),
        (*given, east_west, near, far),
    )
    from_west = lax.ppermute(to_east, "gx", ring("gx", 1))
    from_east = lax.ppermute(to_west, "gx", ring("gx", -1))
    scratch = (pltpu.VMEM((FIELDS, 64, 128), F32), pltpu.VMEM((2, 64, 128), F32))
    early = call(
        west_kernel,
        (
            pltpu.VMEM((128, 128), F32),
            pltpu.VMEM((128, 128), F32),
            pltpu.VMEM((16, 128), F32),
            pltpu.VMEM((32, 128), F32),
            pltpu.VMEM((16, 128), F32),
            pltpu.VMEM((5, 1, 1024), F32),
            pltpu.VMEM((1, 1024), I32),
            pltpu.VMEM((48, 128), F32),
        ),
        (*given, departed, rim, from_west),
        scratch=(*scratch, pltpu.VMEM((4, 16, 256), F32)),
    )
    moist, warm, size, mult, records, box = call(
        east_kernel,
        (
            f32(16, 128),
            f32(16, 128),
            f32(128, 128),
            f32(128, 128),
            f32(5, 1, 2176),
            jax.ShapeDtypeStruct((1, 2176), I32),
        ),
        (*given, departed, rim, from_west, from_east, *early),
        scratch=(
            pltpu.VMEM((16, 128), F32),
            pltpu.VMEM((16, 128), F32),
            pltpu.VMEM((128, 128), F32),
            pltpu.VMEM((128, 128), F32),
            pltpu.VMEM((5, 1, 1152), F32),
            pltpu.VMEM((1, 1152), I32),
            *scratch,
            pltpu.VMEM((4, 8, 256), F32),
            pltpu.SemaphoreType.DMA((8,)),
        ),
        space=pltpu.HBM,
    )
    return (
        moist.reshape(moisture_ratio.shape),
        warm.reshape(kelvin_warmth.shape),
        size.reshape(droplet_size_micron.shape),
        mult.reshape(weighting_factor.shape),
        records,
        box,
    )


def solution(mesh):
    cells = P(None, "gx", "gy")
    drop = P(None, None, "gx", "gy")
    lists = P("gx", None, "gy")
    return jax.shard_map(
        per_device,
        mesh=mesh,
        in_specs=(cells,) * 2 + (drop,) * 6 + (lists,) * 3,
        out_specs=(cells, cells, drop, drop, P(None, "gx", "gy"), P("gx", "gy")),
        check_vma=False,
    )
```
